256 devices in a mesh: blk: 128 (over y, z, x), rep: 2 (over core).
Axes of the slice: x: 4, y: 4, z: 8, core: 2. Of those that a mesh axis runs over, the one named last changes fastest.
Arguments:
- x_points: bfloat16 [131072, 512], P('blk'), may hold values from -8 to 8
- y_points: bfloat16 [131072, 512], P('blk'), may hold values from -8 to 8
- first_masses: float32 [131072], P('blk'), may hold values from 0.25 to 4
- second_masses: float32 [131072], P('blk'), may hold values from 0.25 to 4
- f_start: float32 [131072], P('blk'), may hold values from 0.55 to 20
- g_start: float32 [131072], P('blk'), may hold values from 0.55 to 20
- block_owner: int32 [256], replicated, may hold values from 0 to 255, as said below
- pair_list: int32 [1024, 2], P(('blk', 'rep')), may hold values from -1 to 255, as said below
Outputs:
- f_final: float32 [131072], P('blk')
- g_final: float32 [131072], P('blk')
- mapped_x: bfloat16 [131072, 512], P('blk', 'rep')
- mapped_y: bfloat16 [131072, 512], P('blk', 'rep')
The draws below stay inside these ranges and needn't reach their ends.
Inputs may be any that keep to these rules, and one draw needn't show every extreme that they name: A permutation: block b of either cloud is stored at block position block_owner[b]. `pair_list`: the rows of one index i of blk (those of its devices along rep, in order) begin with 5 to 8 listed pairs and end with rows (-1, -1); some index holds the full 2 * 4 in every draw. A listed pair's first-cloud block has block_owner // 2 = i, its second-cloud block block_owner // 2 = i + d modulo the size of blk, with 1 <= |d| <= 2. No pair is listed twice.
All inputs are finite; a program needn't handle non-finite values.
Results may differ from the reference program's by a relative error of at most 0.0044.
Values may be sent and summed in bfloat16 or wider, within the bound.
A program may use at most 128 MiB of HBM per device.

```python
import math
import jax
import jax.numpy as jnp
from jax import lax

D = 512
BLOCK_POINTS = 512
BLOCKS_PER_SHARD = 2
PAIR_DEV = 4
REACH = 2
BLOCK_TOTAL = 256
NPTS = 131072
PAIRS = 1024
N_BLK = 128
N_REP = 2


def layout(key):
    folded = jax.random.fold_in(key, 7)
    key_owner, key_count, key_order, key_top = jax.random.split(folded, 4)
    owner_map = jax.random.permutation(key_owner, BLOCK_TOTAL).astype(jnp.int32)
    block_of = jnp.zeros((BLOCK_TOTAL,), jnp.int32).at[owner_map].set(jnp.arange(BLOCK_TOTAL, dtype=jnp.int32))
    capacity = PAIR_DEV * N_REP
    count_table = capacity - jnp.array([3, 2, 1, 0, 0], jnp.int32)
    counts = count_table[jax.random.randint(key_count, (N_BLK,), 0, 5)]
    busiest = jax.random.randint(key_top, (), 0, N_BLK)
    counts = counts.at[busiest].set(capacity)
    combos = BLOCKS_PER_SHARD * BLOCKS_PER_SHARD * 2 * REACH
    scores = jax.random.randint(key_order, (N_BLK, combos), 0, 1 << 16) * combos + jnp.arange(combos, dtype=jnp.int32)[None, :]
    ranking = jnp.argsort(scores, axis=1)[:, :capacity].astype(jnp.int32)
    x_pick = ranking % BLOCKS_PER_SHARD
    remainder = ranking // BLOCKS_PER_SHARD
    second = remainder % BLOCKS_PER_SHARD
    step_code = remainder // BLOCKS_PER_SHARD
    offset = jnp.where(step_code < REACH, step_code - REACH, step_code - REACH + 1)
    device = jnp.arange(N_BLK, dtype=jnp.int32)[:, None]
    x_slot = device * BLOCKS_PER_SHARD + x_pick
    y_slot = (device + offset) % N_BLK * BLOCKS_PER_SHARD + second
    is_live = jnp.arange(capacity, dtype=jnp.int32)[None, :] < counts[:, None]
    listed = jnp.stack([jnp.where(is_live, block_of[x_slot], -1), jnp.where(is_live, block_of[y_slot], -1)], axis=-1)
    return (owner_map, listed.reshape(N_BLK * capacity, 2).astype(jnp.int32))


def draw_block_owner(key, part):
    return layout(key)[0]


def draw_pair_list(key, part):
    return layout(key)[1]


def clouds(key):
    key_x, key_y = jax.random.split(jax.random.fold_in(key, 11), 2)
    x_cloud = jnp.clip(jax.random.normal(key_x, (NPTS, D), jnp.float32), -7.5, 7.5)
    y_cloud = jnp.clip(jax.random.normal(key_y, (NPTS, D), jnp.float32), -7.5, 7.5)
    return (x_cloud, y_cloud)


def draw_x_points(key, part):
    return clouds(key)[0].astype(jnp.bfloat16)


def draw_y_points(key, part):
    return clouds(key)[1].astype(jnp.bfloat16)


def potential(key, salt_value):
    values = jax.random.uniform(jax.random.fold_in(key, salt_value), (NPTS,), jnp.float32, 0.55, 0.9)
    return values


def draw_g_start(key, part):
    return potential(key, 17)


def draw_f_start(key, part):
    return potential(key, 19)


def steps_of(key, extent, shards, smallest, top_value):
    factor_of = 1.0
    for axis_at, blocks in shards:
        draws = jax.random.uniform(jax.random.fold_in(jax.random.fold_in(key, 6), axis_at), (blocks,), jnp.float32, smallest / len(shards), top_value / len(shards))
        factor_of = factor_of * jnp.repeat(jnp.exp(draws), extent[axis_at] // blocks).reshape((-1,) + (1,) * (len(extent) - 1 - axis_at))
    return factor_of


def setup_inputs(seed: int = 0) -> dict:
    keys = jax.random.split(jax.random.key(seed), 9)
    x_points = draw_x_points(jax.random.fold_in(keys[8], 71), 0)
    y_points = draw_y_points(jax.random.fold_in(keys[8], 71), 0)
    first_masses = jnp.clip(jnp.exp(math.log(4.0) - 2.7725887 * jax.random.uniform(keys[2], (NPTS,), jnp.float32) ** steps_of(keys[2], (NPTS,), ((0, 128),), -0.2, 0.2)), 0.25, 4.0)
    second_masses = jnp.clip(jnp.exp(math.log(4.0) - 2.7725887 * jax.random.uniform(keys[3], (NPTS,), jnp.float32) ** steps_of(keys[3], (NPTS,), ((0, 128),), -0.2, 0.2)), 0.25, 4.0)
    f_start = draw_f_start(jax.random.fold_in(keys[8], 71), 0)
    g_start = draw_g_start(jax.random.fold_in(keys[8], 71), 0)
    block_owner = draw_block_owner(jax.random.fold_in(keys[8], 71), 0)
    pair_list = draw_pair_list(jax.random.fold_in(keys[8], 71), 0)
    return dict(x_points=x_points, y_points=y_points, first_masses=first_masses, second_masses=second_masses, f_start=f_start, g_start=g_start, block_owner=block_owner, pair_list=pair_list)


entropic_epsilon = 0.05
floor_value = -1.0e30


def block_cost(x_block, y_block):
    x_wide = x_block.astype(jnp.float32)
    y_wide = y_block.astype(jnp.float32)
    x_square = jnp.sum(jnp.square(x_wide), axis=1)
    y_square = jnp.sum(jnp.square(y_wide), axis=1)
    inner_dot = jnp.dot(x_wide, y_wide.T)
    return (x_square[:, None] + y_square[None, :] - 2.0 * inner_dot) / D


def merge_rows(maxima, totals, slot_ids):
    highest = jnp.full((BLOCK_TOTAL, BLOCK_POINTS), floor_value, jnp.float32).at[slot_ids].max(maxima)
    scaled = totals * jnp.exp(maxima - highest[slot_ids])
    combined = jnp.zeros((BLOCK_TOTAL, BLOCK_POINTS), jnp.float32).at[slot_ids].add(scaled)
    return highest + jnp.log(combined)


def reference(x_points, y_points, first_masses, second_masses, f_start, g_start, block_owner, pair_list):
    is_live = pair_list[:, 0] >= 0
    first_id = jnp.where(is_live, pair_list[:, 0], 0).astype(jnp.int32)
    second_id = jnp.where(is_live, pair_list[:, 1], 0).astype(jnp.int32)
    home_slots = jnp.arange(BLOCK_TOTAL, dtype=jnp.int32)
    x_slot = jnp.concatenate([home_slots, block_owner[first_id]]).astype(jnp.int32)
    y_slot = jnp.concatenate([home_slots, block_owner[second_id]]).astype(jnp.int32)
    in_use = jnp.concatenate([jnp.ones((BLOCK_TOTAL,), jnp.bool_), is_live])
    x_blocks = x_points.reshape(BLOCK_TOTAL, BLOCK_POINTS, D)
    y_blocks = y_points.reshape(BLOCK_TOTAL, BLOCK_POINTS, D)
    entries = jnp.arange(BLOCK_TOTAL + PAIRS, dtype=jnp.int32)

    def make_cost(entry_index):
        return block_cost(x_blocks[x_slot[entry_index]], y_blocks[y_slot[entry_index]])

    cost_tiles = lax.map(make_cost, entries)
    first_log_mass = entropic_epsilon * jnp.log(first_masses.reshape(BLOCK_TOTAL, BLOCK_POINTS))
    second_log_mass = entropic_epsilon * jnp.log(second_masses.reshape(BLOCK_TOTAL, BLOCK_POINTS))

    def softmin_parts(first_block_start, second_block_start):
        def one_entry(packed):
            pair_cost_block, first_block_index, second_block_index, active = packed
            row_logits = (second_block_start[second_block_index][None, :] - pair_cost_block) / entropic_epsilon
            column_logits = (first_block_start[first_block_index][:, None] - pair_cost_block) / entropic_epsilon
            row_high = jnp.max(row_logits, axis=1)
            col_high = jnp.max(column_logits, axis=0)
            row_summed = jnp.sum(jnp.exp(row_logits - row_high[:, None]), axis=1)
            col_summed = jnp.sum(jnp.exp(column_logits - col_high[None, :]), axis=0)
            return (jnp.where(active, row_high, floor_value), jnp.where(active, row_summed, 0.0),
                    jnp.where(active, col_high, floor_value), jnp.where(active, col_summed, 0.0))

        row_high, row_summed, col_high, col_summed = lax.map(one_entry, (cost_tiles, x_slot, y_slot, in_use))
        return merge_rows(row_high, row_summed, x_slot), merge_rows(col_high, col_summed, y_slot)

    first_potential = f_start.reshape(BLOCK_TOTAL, BLOCK_POINTS)
    second_potential = g_start.reshape(BLOCK_TOTAL, BLOCK_POINTS)
    for sweep_count in range(2):
        row_logsumexp, column_logsumexp = softmin_parts(first_potential + first_log_mass, second_potential + second_log_mass)
        first_potential, second_potential = 0.5 * (first_potential - entropic_epsilon * row_logsumexp), 0.5 * (second_potential - entropic_epsilon * column_logsumexp)
    first_block_start = first_potential + first_log_mass
    second_block_start = second_potential + second_log_mass
    row_logsumexp, column_logsumexp = softmin_parts(first_block_start, second_block_start)

    def accumulate(carried, packed):
        x_sums, y_sums = carried
        pair_cost_block, first_block_index, second_block_index, active = packed
        row_factor = jnp.exp((second_block_start[second_block_index][None, :] - pair_cost_block) / entropic_epsilon - row_logsumexp[first_block_index][:, None])
        column_factor = jnp.exp((first_block_start[first_block_index][:, None] - pair_cost_block) / entropic_epsilon - column_logsumexp[second_block_index][None, :])
        row_factor = jnp.where(active, row_factor, 0.0).astype(jnp.bfloat16).astype(jnp.float32)
        column_factor = jnp.where(active, column_factor, 0.0).astype(jnp.bfloat16).astype(jnp.float32)
        add_x = jnp.dot(row_factor, y_blocks[second_block_index].astype(jnp.float32))
        add_y = jnp.dot(column_factor.T, x_blocks[first_block_index].astype(jnp.float32))
        return (x_sums.at[first_block_index].add(add_x), y_sums.at[second_block_index].add(add_y)), None

    zeros_sums = jnp.zeros((BLOCK_TOTAL, BLOCK_POINTS, D), jnp.float32)
    (x_sums, y_sums), unused = lax.scan(accumulate, (zeros_sums, zeros_sums), (cost_tiles, x_slot, y_slot, in_use))
    return (first_potential.reshape(NPTS), second_potential.reshape(NPTS),
            x_sums.reshape(NPTS, D).astype(jnp.bfloat16), y_sums.reshape(NPTS, D).astype(jnp.bfloat16))
```

```python
import functools
import math

import jax
import jax.numpy as jnp
from jax import lax
from jax.experimental import pallas as pl
from jax.experimental.pallas import tpu as pltpu
from jax.sharding import PartitionSpec as P

D = 512
BLOCK = 512
LANES = 128
GROUPS = BLOCK // LANES
TILES = 9
PAIR_DEV = 4
OFFSETS = (-1, 1, -2, 2)
MIRROR = (1, 0, 3, 2)
PEERS = 9

epsilon = 0.05
K2 = 1.0 / (epsilon * math.log(2.0))
INV_LN2 = 1.0 / math.log(2.0)
NEG = -1.0e30
MESH = pl.DeviceIdType.MESH


def kernel(
    n, pair_ref, owner_ref, x_hbm, y_hbm, m1_ref, m2_ref, f0_ref, g0_ref,
    f_out, g_out, mx_out, my_out,
    own, win, scores, bvec, bias, mpart, spart, lrow, lcol, acc, obuf,
    pot, nrm, lmass, first, ibuf, tile, mbuf,
    load_sem, bsend, brecv, csend, crecv, isend, irecv, psend, precv, osend, orecv,
):
    i = lax.axis_index("blk")
    r = lax.axis_index("rep")
    other = 1 - r

    def chip(offset):
        return lax.rem(i + (n + offset), n)

    def rdma(src, dst, send, recv, where):
        return pltpu.make_async_remote_copy(
            src_ref=src, dst_ref=dst, send_sem=send, recv_sem=recv,
            device_id=where, device_id_type=MESH,
        )

    peers = [(chip(OFFSETS[s]), q) for s in range(4) for q in range(2)] + [(i, other)]

    rows = pl.ds(pl.multiple_of(r * BLOCK, BLOCK), BLOCK)
    load_y = pltpu.make_async_copy(y_hbm.at[rows, :], own.at[0], load_sem.at[0])
    load_x = pltpu.make_async_copy(x_hbm.at[rows, :], own.at[1], load_sem.at[1])
    load_y.start()
    load_x.start()

    barrier = pltpu.get_barrier_semaphore()
    for peer in peers:
        pl.semaphore_signal(barrier, inc=1, device_id=peer, device_id_type=MESH)
    pl.semaphore_wait(barrier, PEERS)

    def step_copy(t, slot):
        ahead = chip(1) if slot % 2 == 0 else chip(-1)
        src = own.at[t] if slot < 2 else win.at[t, slot - 2, r]
        return rdma(src, win.at[t, slot, r], bsend.at[t, slot], brecv.at[t, slot], (ahead, r))

    def cross_copy(t, slot, piece):
        return rdma(
            win.at[t, slot, piece], win.at[t, slot, piece],
            csend.at[t, slot], crecv.at[t, slot], (i, other),
        )

    load_y.wait()
    step_copy(0, 0).start()
    step_copy(0, 1).start()
    load_x.wait()

    pot[0] = g0_ref[r]
    pot[1] = f0_ref[r]
    lmass[0] = jnp.log(m2_ref[r]) * INV_LN2
    lmass[1] = jnp.log(m1_ref[r]) * INV_LN2

    def spread(row, store):
        for l in range(GROUPS):
            store[l : l + 1, :] = row[:, l * LANES : (l + 1) * LANES]

    for t in range(2):
        def square(g, _):
            at = pl.ds(pl.multiple_of(g * 64, 64), 64)
            v = own[t, at, :].astype(jnp.float32)
            v = v * v
            part = v[:, 0:LANES]
            for l in range(1, GROUPS):
                part = part + v[:, l * LANES : (l + 1) * LANES]
            mpart[at, :] = part
            return 0

        lax.fori_loop(0, BLOCK // 64, square, 0)
        total = jnp.sum(jnp.transpose(mpart[...]), axis=0, keepdims=True)
        spread(total * (1.0 / D), lrow)
        nrm[t] = lrow[0:GROUPS, :]
        first[t, 0:GROUPS, :] = K2 * (pot[t] - nrm[t]) + lmass[t]
        first[t, GROUPS : 2 * GROUPS, :] = pot[t]

    line = lax.broadcasted_iota(jnp.int32, (8, LANES), 0)
    listed = jnp.zeros((8, LANES), jnp.float32)
    for p in range(PAIR_DEV):
        a_id = pair_ref[p, 0]
        c_id = pair_ref[p, 1]
        x_at = owner_ref[jnp.maximum(a_id, 0)]
        y_at = owner_ref[jnp.maximum(c_id, 0)]
        offset = lax.rem((y_at >> 1) - i + (n + 2), n) - 2
        slot = jnp.where(offset == -1, 0, jnp.where(offset == 1, 1, jnp.where(offset == -2, 2, 3)))
        at = jnp.where(a_id >= 0, slot * 2 + (y_at & 1), -1)
        amount = ((x_at & 1) + 1).astype(jnp.float32)
        listed = listed + jnp.where(line == at, amount, 0.0)
    first[2] = listed

    def first_copy(k):
        back = MIRROR[k // 2] * 2 + r if k < 8 else 8
        return rdma(first, ibuf.at[back], isend.at[k], irecv.at[back], peers[k])

    def first_wait(k):
        rdma(first, ibuf.at[k], isend.at[k], irecv.at[k], peers[k]).wait_recv()

    for k in range(PEERS):
        first_copy(k).start()
    step_copy(1, 0).start()
    step_copy(1, 1).start()

    def put_scores(side, p, keys):
        dot = lax.dot_general(
            own[1 - side], keys, (((1,), (1,)), ((), ())), preferred_element_type=jnp.float32
        )
        scores[side, p] = dot * (2.0 * K2 / D)

    def home_side(side, _):
        put_scores(side, 0, own[side])
        return 0

    lax.fori_loop(0, 2, home_side, 0)

    def window_scores(side, base):
        def one(j, _):
            put_scores(side, 1 + base * 2 + j, win[side, base + j // 2, j % 2])
            return 0

        lax.fori_loop(0, 4, one, 0)

    def arrive(t, base):
        for slot in (base, base + 1):
            step_copy(t, slot).wait_recv()
            if base == 0:
                step_copy(t, slot + 2).start()
            cross_copy(t, slot, r).start()

    def arrive_cross(t, base):
        for slot in (base, base + 1):
            cross_copy(t, slot, other).wait_recv()

    arrive(0, 0)
    arrive_cross(0, 0)
    window_scores(0, 0)
    arrive(1, 0)
    arrive_cross(1, 0)
    window_scores(1, 0)

    for k in range(PEERS):
        first_wait(k)

    def allow(v, block):
        low = jnp.where(v == 1.0, 0.0, jnp.where(v == 3.0, 0.0, NEG))
        high = jnp.where(v >= 2.0, 0.0, NEG)
        if isinstance(block, int):
            return low if block == 0 else high
        return jnp.where(block == 0, low, high)

    mine = first[2] + ibuf[8, 2]
    bias[0] = allow(mine, r)
    for s in range(4):
        theirs = ibuf[2 * s, 2] + ibuf[2 * s + 1, 2]
        at = MIRROR[s] * 2
        v = jnp.where(r == 0, theirs[at : at + 1, :], theirs[at + 1 : at + 2, :])
        for q in range(2):
            bias[1, 2 * s + q : 2 * s + q + 1, :] = allow(v, q)

    def put_vector(side, home, source):
        for p in range(TILES):
            ref = home if p == 0 else source(p - 1)
            for l in range(GROUPS):
                row = ref[l : l + 1, :]
                if p > 0:
                    row = row + bias[side, p - 1 : p, :]
                at = (p * GROUPS + l) * LANES
                bvec[side, :, at : at + LANES] = jnp.broadcast_to(row, (8, LANES))

    def lse_pass(side):
        def group(g, _):
            at = pl.ds(pl.multiple_of(g * 8, 8), 8)
            terms = []
            for p in range(TILES):
                for l in range(GROUPS):
                    o = (p * GROUPS + l) * LANES
                    terms.append(
                        scores[side, p, at, l * LANES : (l + 1) * LANES]
                        + bvec[side, :, o : o + LANES]
                    )
            highs = [functools.reduce(jnp.maximum, terms[h::4]) for h in range(4)]
            high = jnp.maximum(jnp.maximum(highs[0], highs[1]), jnp.maximum(highs[2], highs[3]))
            sums = [sum(jnp.exp2(t - high) for t in terms[h::4]) for h in range(4)]
            mpart[at, :] = high
            spart[at, :] = (sums[0] + sums[1]) + (sums[2] + sums[3])
            return 0

        lax.fori_loop(0, BLOCK // 8, group, 0)

    def update(side, step):
        t = 1 - side
        turned = jnp.transpose(mpart[...])
        high = jnp.max(turned, axis=0, keepdims=True)
        total = jnp.sum(jnp.transpose(spart[...]) * jnp.exp2(turned - high), axis=0, keepdims=True)
        spread(high + jnp.log(total) * INV_LN2, lrow)
        new = 0.5 * (pot[t] - lrow[0:GROUPS, :] * (1.0 / K2) + nrm[t])
        pot[t] = new
        tile[step, t, 0:GROUPS, :] = K2 * (new - nrm[t]) + lmass[t]
        tile[step, t, GROUPS : 2 * GROUPS, :] = new

    def tile_copy(step, t, k):
        back = MIRROR[k // 2] * 2 + r if k < 8 else 8
        return rdma(
            tile.at[step, t], mbuf.at[step, t, back],
            psend.at[step, t, k], precv.at[step, t, back], peers[k],
        )

    def send_tiles(step, t):
        for k in range(PEERS):
            tile_copy(step, t, k).start()

    def take_tiles(step, t):
        for k in range(PEERS):
            rdma(
                tile.at[step, t], mbuf.at[step, t, k],
                psend.at[step, t, k], precv.at[step, t, k], peers[k],
            ).wait_recv()
        put_vector(t, tile.at[step, t], lambda k: mbuf.at[step, t, k])

    arrive(0, 2)
    arrive_cross(0, 2)
    window_scores(0, 2)
    put_vector(0, first.at[0], lambda k: ibuf.at[k, 0])
    lse_pass(0)
    update(0, 0)
    send_tiles(0, 1)

    arrive(1, 2)
    arrive_cross(1, 2)
    window_scores(1, 2)
    put_vector(1, first.at[1], lambda k: ibuf.at[k, 1])
    lse_pass(1)
    update(1, 0)
    send_tiles(0, 0)

    take_tiles(0, 1)
    lse_pass(1)
    update(1, 1)
    send_tiles(1, 0)

    take_tiles(0, 0)
    lse_pass(0)
    update(0, 1)
    send_tiles(1, 1)

    f_out[r] = pot[1]
    g_out[r] = pot[0]

    def out_copy(side):
        dst = (mx_out, my_out)[side]
        return rdma(obuf.at[side], dst.at[r], osend.at[side], orecv.at[side], (i, other))

    def final(side, out_ref):
        lse_pass(side)

        def column(g, _):
            at = pl.ds(pl.multiple_of(g * 64, 64), 64)
            part = mpart[at, :]
            high = jnp.max(part, axis=1, keepdims=True)
            total = jnp.sum(spart[at, :] * jnp.exp2(part - high), axis=1, keepdims=True)
            lcol[at, :] = jnp.broadcast_to(high + jnp.log(total) * INV_LN2, (64, LANES))
            return 0

        lax.fori_loop(0, BLOCK // 64, column, 0)

        def weigh(p, keys):
            pieces = []
            for l in range(GROUPS):
                o = pl.multiple_of(p * BLOCK + l * LANES, LANES)
                v = scores[side, p, :, l * LANES : (l + 1) * LANES]
                v = v + bvec[side, 0:1, pl.ds(o, LANES)]
                pieces.append(jnp.exp2(v - lcol[...]).astype(jnp.bfloat16))
            return jnp.dot(
                jnp.concatenate(pieces, axis=1), keys, preferred_element_type=jnp.float32
            )

        acc[...] = weigh(0, own[side])

        def one(j, _):
            acc[...] += weigh(j + 1, win[side, j // 2, j % 2])
            return 0

        lax.fori_loop(0, 8, one, 0)
        half = D // 2
        low = acc[:, 0:half].astype(jnp.bfloat16)
        high = acc[:, half:D].astype(jnp.bfloat16)
        obuf[side] = jnp.where(r == 0, high, low)
        out_copy(side).start()
        out_ref[r] = jnp.where(r == 0, low, high)

    take_tiles(1, 0)
    final(0, mx_out)
    take_tiles(1, 1)
    g_out[other] = mbuf[1, 0, 8, GROUPS : 2 * GROUPS, :]
    f_out[other] = mbuf[1, 1, 8, GROUPS : 2 * GROUPS, :]
    final(1, my_out)

    for side in range(2):
        dst = (mx_out, my_out)[side]
        rdma(
            obuf.at[side], dst.at[other], osend.at[side], orecv.at[side], (i, other)
        ).wait_recv()
        out_copy(side).wait_send()
    for t in range(2):
        for slot in range(4):
            step_copy(t, slot).wait_send()
            cross_copy(t, slot, r).wait_send()
    for k in range(PEERS):
        first_copy(k).wait_send()
        for step in range(2):
            for t in range(2):
                tile_copy(step, t, k).wait_send()


def per_device(
    x_points, y_points, first_masses, second_masses, f_start, g_start, block_owner, pair_list
):
    n = lax.axis_size("blk")
    shape = (2, GROUPS, LANES)
    f32, bf16 = jnp.float32, jnp.bfloat16
    dma = pltpu.SemaphoreType.DMA
    smem = pl.BlockSpec(memory_space=pltpu.SMEM)
    vmem = pl.BlockSpec(memory_space=pltpu.VMEM)
    hbm = pl.BlockSpec(memory_space=pl.ANY)
    f, g, mx, my = pl.pallas_call(
        functools.partial(kernel, n),
        out_shape=(
            jax.ShapeDtypeStruct(shape, f32),
            jax.ShapeDtypeStruct(shape, f32),
            jax.ShapeDtypeStruct((2, BLOCK, D // 2), bf16),
            jax.ShapeDtypeStruct((2, BLOCK, D // 2), bf16),
        ),
        in_specs=[smem, smem, hbm, hbm, vmem, vmem, vmem, vmem],
        out_specs=(vmem, vmem, vmem, vmem),
        scratch_shapes=[
            pltpu.VMEM((2, BLOCK, D), bf16),
            pltpu.VMEM((2, 4, 2, BLOCK, D), bf16),
            pltpu.VMEM((2, TILES, BLOCK, BLOCK), f32),
            pltpu.VMEM((2, 8, TILES * BLOCK), f32),
            pltpu.VMEM((2, 8, LANES), f32),
            pltpu.VMEM((BLOCK, LANES), f32),
            pltpu.VMEM((BLOCK, LANES), f32),
            pltpu.VMEM((8, LANES), f32),
            pltpu.VMEM((BLOCK, LANES), f32),
            pltpu.VMEM((BLOCK, D), f32),
            pltpu.VMEM((2, BLOCK, D // 2), bf16),
            pltpu.VMEM(shape, f32),
            pltpu.VMEM(shape, f32),
            pltpu.VMEM(shape, f32),
            pltpu.VMEM((3, 8, LANES), f32),
            pltpu.VMEM((PEERS, 3, 8, LANES), f32),
            pltpu.VMEM((2, 2, 8, LANES), f32),
            pltpu.VMEM((2, 2, PEERS, 8, LANES), f32),
            dma((2,)),
            dma((2, 4)),
            dma((2, 4)),
            dma((2, 4)),
            dma((2, 4)),
            dma((PEERS,)),
            dma((PEERS,)),
            dma((2, 2, PEERS)),
            dma((2, 2, PEERS)),
            dma((2,)),
            dma((2,)),
        ],
        compiler_params=pltpu.CompilerParams(
            collective_id=0, has_side_effects=True, vmem_limit_bytes=60 * 1024 * 1024
        ),
    )(
        pair_list, block_owner, x_points, y_points,
        first_masses.reshape(shape), second_masses.reshape(shape),
        f_start.reshape(shape), g_start.reshape(shape),
    )
    rows = 2 * BLOCK
    return f.reshape(rows), g.reshape(rows), mx.reshape(rows, D // 2), my.reshape(rows, D // 2)


def solution(mesh):
    placed = (
        P("blk", None),
        P("blk", None),
        P("blk"),
        P("blk"),
        P("blk"),
        P("blk"),
        P(),
        P(("blk", "rep"), None),
    )
    return jax.shard_map(
        per_device,
        mesh=mesh,
        in_specs=placed,
        out_specs=(P("blk"), P("blk"), P("blk", "rep"), P("blk", "rep")),
        check_vma=False,
    )
```

```python
import functools
import math

import jax
import jax.numpy as jnp
from jax import lax
from jax.experimental import pallas as pl
from jax.experimental.pallas import tpu as pltpu
from jax.sharding import PartitionSpec as P

D = 512
BLOCK = 512
LANES = 128
GROUPS = BLOCK // LANES
TILES = 9
PAIR_DEV = 4
OFFSETS = (-1, 1, -2, 2)
MIRROR = (1, 0, 3, 2)
PEERS = 9

epsilon = 0.05
K2 = 1.0 / (epsilon * math.log(2.0))
INV_LN2 = 1.0 / math.log(2.0)
NEG = -1.0e30
MESH = pl.DeviceIdType.MESH


def kernel(
    n, pair_ref, owner_ref, x_hbm, y_hbm, m1_ref, m2_ref, f0_ref, g0_ref,
    f_out, g_out, mx_out, my_out,
    own, win, scores, bvec, bias, mpart, spart, lrow, lcol, acc, obuf,
    pot, nrm, lmass, first, ibuf, tile, mbuf,
    load_sem, bsend, brecv, csend, crecv, isend, irecv, psend, precv, osend, orecv,
):
    i = lax.axis_index("blk")
    r = lax.axis_index("rep")
    other = 1 - r

    def chip(offset):
        return lax.rem(i + (n + offset), n)

    def rdma(src, dst, send, recv, where):
        return pltpu.make_async_remote_copy(
            src_ref=src, dst_ref=dst, send_sem=send, recv_sem=recv,
            device_id=where, device_id_type=MESH,
        )

    peers = [(chip(OFFSETS[s]), q) for s in range(4) for q in range(2)] + [(i, other)]

    rows = pl.ds(pl.multiple_of(r * BLOCK, BLOCK), BLOCK)
    load_y = pltpu.make_async_copy(y_hbm.at[rows, :], own.at[0], load_sem.at[0])
    load_x = pltpu.make_async_copy(x_hbm.at[rows, :], own.at[1], load_sem.at[1])
    load_y.start()
    load_x.start()

    barrier = pltpu.get_barrier_semaphore()
    for peer in peers:
        pl.semaphore_signal(barrier, inc=1, device_id=peer, device_id_type=MESH)
    pl.semaphore_wait(barrier, PEERS)

    def step_copy(t, slot):
        ahead = chip(1) if slot % 2 == 0 else chip(-1)
        src = own.at[t] if slot < 2 else win.at[t, slot - 2, r]
        return rdma(src, win.at[t, slot, r], bsend.at[t, slot], brecv.at[t, slot], (ahead, r))

    def cross_copy(t, slot, piece):
        return rdma(
            win.at[t, slot, piece], win.at[t, slot, piece],
            csend.at[t, slot], crecv.at[t, slot], (i, other),
        )

    load_y.wait()
    step_copy(0, 0).start()
    step_copy(0, 1).start()
    load_x.wait()

    pot[0] = g0_ref[r]
    pot[1] = f0_ref[r]
    lmass[0] = jnp.log(m2_ref[r]) * INV_LN2
    lmass[1] = jnp.log(m1_ref[r]) * INV_LN2

    def spread(row, store):
        for l in range(GROUPS):
            store[l : l + 1, :] = row[:, l * LANES : (l + 1) * LANES]

    for t in range(2):
        def square(g, _):
            at = pl.ds(pl.multiple_of(g * 64, 64), 64)
            v = own[t, at, :].astype(jnp.float32)
            v = v * v
            part = v[:, 0:LANES]
            for l in range(1, GROUPS):
                part = part + v[:, l * LANES : (l + 1) * LANES]
            mpart[at, :] = part
            return 0

        lax.fori_loop(0, BLOCK // 64, square, 0)
        total = jnp.sum(jnp.transpose(mpart[...]), axis=0, keepdims=True)
        spread(total * (1.0 / D), lrow)
        nrm[t] = lrow[0:GROUPS, :]
        first[t, 0:GROUPS, :] = K2 * (pot[t] - nrm[t]) + lmass[t]
        first[t, GROUPS : 2 * GROUPS, :] = pot[t]

    line = lax.broadcasted_iota(jnp.int32, (8, LANES), 0)
    listed = jnp.zeros((8, LANES), jnp.float32)
    for p in range(PAIR_DEV):
        a_id = pair_ref[0, p]
        c_id = pair_ref[1, p]
        x_at = owner_ref[jnp.maximum(a_id, 0)]
        y_at = owner_ref[jnp.maximum(c_id, 0)]
        offset = lax.rem((y_at >> 1) - i + (n + 2), n) - 2
        slot = jnp.where(offset == -1, 0, jnp.where(offset == 1, 1, jnp.where(offset == -2, 2, 3)))
        at = jnp.where(a_id >= 0, slot * 2 + (y_at & 1), -1)
        amount = ((x_at & 1) + 1).astype(jnp.float32)
        listed = listed + jnp.where(line == at, amount, 0.0)
    first[2] = listed

    def first_copy(k):
        back = MIRROR[k // 2] * 2 + r if k < 8 else 8
        return rdma(first, ibuf.at[back], isend.at[k], irecv.at[back], peers[k])

    def first_wait(k):
        rdma(first, ibuf.at[k], isend.at[k], irecv.at[k], peers[k]).wait_recv()

    for k in range(PEERS):
        first_copy(k).start()
    step_copy(1, 0).start()
    step_copy(1, 1).start()

    def put_scores(side, p, keys):
        dot = lax.dot_general(
            own[1 - side], keys, (((1,), (1,)), ((), ())), preferred_element_type=jnp.float32
        )
        scores[side, p] = dot * (2.0 * K2 / D)

    def home_side(side, _):
        put_scores(side, 0, own[side])
        return 0

    lax.fori_loop(0, 2, home_side, 0)

    def window_scores(side, base):
        def one(j, _):
            put_scores(side, 1 + base * 2 + j, win[side, base + j // 2, j % 2])
            return 0

        lax.fori_loop(0, 4, one, 0)

    def arrive(t, base):
        for slot in (base, base + 1):
            step_copy(t, slot).wait_recv()
            if base == 0:
                step_copy(t, slot + 2).start()
            cross_copy(t, slot, r).start()

    def arrive_cross(t, base):
        for slot in (base, base + 1):
            cross_copy(t, slot, other).wait_recv()

    arrive(0, 0)
    arrive_cross(0, 0)
    window_scores(0, 0)
    arrive(1, 0)
    arrive_cross(1, 0)
    window_scores(1, 0)

    for k in range(PEERS):
        first_wait(k)

    def allow(v, block):
        low = jnp.where(v == 1.0, 0.0, jnp.where(v == 3.0, 0.0, NEG))
        high = jnp.where(v >= 2.0, 0.0, NEG)
        if isinstance(block, int):
            return low if block == 0 else high
        return jnp.where(block == 0, low, high)

    mine = first[2] + ibuf[8, 2]
    bias[0] = allow(mine, r)
    for s in range(4):
        theirs = ibuf[2 * s, 2] + ibuf[2 * s + 1, 2]
        at = MIRROR[s] * 2
        v = jnp.where(r == 0, theirs[at : at + 1, :], theirs[at + 1 : at + 2, :])
        for q in range(2):
            bias[1, 2 * s + q : 2 * s + q + 1, :] = allow(v, q)

    def put_vector(side, home, source):
        for p in range(TILES):
            ref = home if p == 0 else source(p - 1)
            for l in range(GROUPS):
                row = ref[l : l + 1, :]
                if p > 0:
                    row = row + bias[side, p - 1 : p, :]
                at = (p * GROUPS + l) * LANES
                bvec[side, :, at : at + LANES] = jnp.broadcast_to(row, (8, LANES))

    def lse_pass(side, tiles=range(TILES), merge=False):
        def group(g, _):
            at = pl.ds(pl.multiple_of(g * 32, 32), 32)

            def term(o):
                b = bvec[side, :, o * LANES : (o + 1) * LANES]
                p, l = divmod(o, GROUPS)
                v = scores[side, p, at, l * LANES : (l + 1) * LANES]
                return v + jnp.concatenate([b] * 4, axis=0)

            spots = [p * GROUPS + l for p in tiles for l in range(GROUPS)]
            high = jnp.maximum(
                functools.reduce(jnp.maximum, [term(o) for o in spots[0::2]]),
                functools.reduce(jnp.maximum, [term(o) for o in spots[1::2]]),
            )
            if merge:
                high = jnp.maximum(high, mpart[at, :])
            total = sum(jnp.exp2(term(o) - high) for o in spots[0::2])
            total = total + sum(jnp.exp2(term(o) - high) for o in spots[1::2])
            if merge:
                total = total + spart[at, :] * jnp.exp2(mpart[at, :] - high)
            mpart[at, :] = high
            spart[at, :] = total
            return 0

        lax.fori_loop(0, BLOCK // 32, group, 0)

    def update(side, step):
        t = 1 - side
        turned = jnp.transpose(mpart[...])
        high = jnp.max(turned, axis=0, keepdims=True)
        total = jnp.sum(jnp.transpose(spart[...]) * jnp.exp2(turned - high), axis=0, keepdims=True)
        spread(high + jnp.log(total) * INV_LN2, lrow)
        new = 0.5 * (pot[t] - lrow[0:GROUPS, :] * (1.0 / K2) + nrm[t])
        pot[t] = new
        tile[step, t, 0:GROUPS, :] = K2 * (new - nrm[t]) + lmass[t]
        tile[step, t, GROUPS : 2 * GROUPS, :] = new

    def tile_copy(step, t, k):
        back = MIRROR[k // 2] * 2 + r if k < 8 else 8
        return rdma(
            tile.at[step, t], mbuf.at[step, t, back],
            psend.at[step, t, k], precv.at[step, t, back], peers[k],
        )

    def send_tiles(step, t):
        for k in range(PEERS):
            tile_copy(step, t, k).start()

    def take_tiles(step, t):
        for k in range(PEERS):
            rdma(
                tile.at[step, t], mbuf.at[step, t, k],
                psend.at[step, t, k], precv.at[step, t, k], peers[k],
            ).wait_recv()
        put_vector(t, tile.at[step, t], lambda k: mbuf.at[step, t, k])

    arrive(0, 2)
    arrive_cross(0, 2)
    window_scores(0, 2)
    put_vector(0, first.at[0], lambda k: ibuf.at[k, 0])
    lse_pass(0)
    update(0, 0)
    send_tiles(0, 1)

    arrive(1, 2)
    arrive_cross(1, 2)
    window_scores(1, 2)
    put_vector(1, first.at[1], lambda k: ibuf.at[k, 1])
    lse_pass(1)
    update(1, 0)
    send_tiles(0, 0)

    take_tiles(0, 1)
    lse_pass(1)
    update(1, 1)
    send_tiles(1, 0)

    take_tiles(0, 0)
    lse_pass(0)
    update(0, 1)
    send_tiles(1, 1)

    f_out[r] = pot[1]
    g_out[r] = pot[0]

    def out_copy(side):
        dst = (mx_out, my_out)[side]
        return rdma(obuf.at[side], dst.at[r], osend.at[side], orecv.at[side], (i, other))

    def final(side, out_ref):
        lse_pass(side)

        def column(g, _):
            at = pl.ds(pl.multiple_of(g * 64, 64), 64)
            part = mpart[at, :]
            high = jnp.max(part, axis=1, keepdims=True)
            total = jnp.sum(spart[at, :] * jnp.exp2(part - high), axis=1, keepdims=True)
            lcol[at, :] = jnp.broadcast_to(high + jnp.log(total) * INV_LN2, (64, LANES))
            return 0

        lax.fori_loop(0, BLOCK // 64, column, 0)

        def weigh(p, keys):
            pieces = []
            for l in range(GROUPS):
                o = pl.multiple_of(p * BLOCK + l * LANES, LANES)
                v = scores[side, p, :, l * LANES : (l + 1) * LANES]
                v = v + bvec[side, 0:1, pl.ds(o, LANES)]
                pieces.append(jnp.exp2(v - lcol[...]).astype(jnp.bfloat16))
            return jnp.dot(
                jnp.concatenate(pieces, axis=1), keys, preferred_element_type=jnp.float32
            )

        acc[...] = weigh(0, own[side])

        def one(j, _):
            acc[...] += weigh(j + 1, win[side, j // 2, j % 2])
            return 0

        lax.fori_loop(0, 8, one, 0)
        half = D // 2
        low = acc[:, 0:half].astype(jnp.bfloat16)
        high = acc[:, half:D].astype(jnp.bfloat16)
        obuf[side] = jnp.where(r == 0, high, low)
        out_copy(side).start()
        out_ref[r] = jnp.where(r == 0, low, high)

    take_tiles(1, 0)
    final(0, mx_out)
    take_tiles(1, 1)
    g_out[other] = mbuf[1, 0, 8, GROUPS : 2 * GROUPS, :]
    f_out[other] = mbuf[1, 1, 8, GROUPS : 2 * GROUPS, :]
    final(1, my_out)

    for side in range(2):
        dst = (mx_out, my_out)[side]
        rdma(
            obuf.at[side], dst.at[other], osend.at[side], orecv.at[side], (i, other)
        ).wait_recv()
        out_copy(side).wait_send()
    for t in range(2):
        for slot in range(4):
            step_copy(t, slot).wait_send()
            cross_copy(t, slot, r).wait_send()
    for k in range(PEERS):
        first_copy(k).wait_send()
        for step in range(2):
            for t in range(2):
                tile_copy(step, t, k).wait_send()


def emit(*refs):
    sources, sinks, rooms, (come, go) = refs[0:4], refs[4:8], refs[8:12], refs[12:14]
    into = [pltpu.make_async_copy(sources[k], rooms[k], come.at[k]) for k in range(4)]
    out = [pltpu.make_async_copy(rooms[k], sinks[k], go.at[k]) for k in range(4)]
    for copy in into:
        copy.start()
    for k in range(4):
        into[k].wait()
        out[k].start()
    for copy in out:
        copy.wait()


def per_device(
    x_points, y_points, first_masses, second_masses, f_start, g_start, block_owner, pair_list
):
    n = lax.axis_size("blk")
    shape = (2, GROUPS, LANES)
    f32, bf16 = jnp.float32, jnp.bfloat16
    dma = pltpu.SemaphoreType.DMA
    smem = pl.BlockSpec(memory_space=pltpu.SMEM)
    vmem = pl.BlockSpec(memory_space=pltpu.VMEM)
    hbm = pl.BlockSpec(memory_space=pl.ANY)
    f, g, mx, my = pl.pallas_call(
        functools.partial(kernel, n),
        out_shape=(
            jax.ShapeDtypeStruct(shape, f32),
            jax.ShapeDtypeStruct(shape, f32),
            jax.ShapeDtypeStruct((2, BLOCK, D // 2), bf16),
            jax.ShapeDtypeStruct((2, BLOCK, D // 2), bf16),
        ),
        in_specs=[smem, smem, hbm, hbm, vmem, vmem, vmem, vmem],
        out_specs=(vmem, vmem, vmem, vmem),
        scratch_shapes=[
            pltpu.VMEM((2, BLOCK, D), bf16),
            pltpu.VMEM((2, 4, 2, BLOCK, D), bf16),
            pltpu.VMEM((2, TILES, BLOCK, BLOCK), f32),
            pltpu.VMEM((2, 8, TILES * BLOCK), f32),
            pltpu.VMEM((2, 8, LANES), f32),
            pltpu.VMEM((BLOCK, LANES), f32),
            pltpu.VMEM((BLOCK, LANES), f32),
            pltpu.VMEM((8, LANES), f32),
            pltpu.VMEM((BLOCK, LANES), f32),
            pltpu.VMEM((BLOCK, D), f32),
            pltpu.VMEM((2, BLOCK, D // 2), bf16),
            pltpu.VMEM(shape, f32),
            pltpu.VMEM(shape, f32),
            pltpu.VMEM(shape, f32),
            pltpu.VMEM((3, 8, LANES), f32),
            pltpu.VMEM((PEERS, 3, 8, LANES), f32),
            pltpu.VMEM((2, 2, 8, LANES), f32),
            pltpu.VMEM((2, 2, PEERS, 8, LANES), f32),
            dma((2,)),
            dma((2, 4)),
            dma((2, 4)),
            dma((2, 4)),
            dma((2, 4)),
            dma((PEERS,)),
            dma((PEERS,)),
            dma((2, 2, PEERS)),
            dma((2, 2, PEERS)),
            dma((2,)),
            dma((2,)),
        ],
        compiler_params=pltpu.CompilerParams(
            collective_id=0, has_side_effects=True, vmem_limit_bytes=63 * 1024 * 1024
        ),
    )(
        pair_list.T, block_owner, x_points, y_points,
        first_masses.reshape(shape), second_masses.reshape(shape),
        f_start.reshape(shape), g_start.reshape(shape),
    )
    f, g, mx, my = pl.pallas_call(
        emit,
        out_shape=tuple(jax.ShapeDtypeStruct(a.shape, a.dtype) for a in (f, g, mx, my)),
        in_specs=[hbm] * 4,
        out_specs=(hbm,) * 4,
        scratch_shapes=[pltpu.VMEM(a.shape, a.dtype) for a in (f, g, mx, my)] + [dma((4,))] * 2,
        compiler_params=pltpu.CompilerParams(vmem_limit_bytes=63 * 1024 * 1024),
    )(f, g, mx, my)
    rows = 2 * BLOCK
    return f.reshape(rows), g.reshape(rows), mx.reshape(rows, D // 2), my.reshape(rows, D // 2)


def solution(mesh):
    placed = (
        P("blk", None),
        P("blk", None),
        P("blk"),
        P("blk"),
        P("blk"),
        P("blk"),
        P(),
        P(("blk", "rep"), None),
    )
    return jax.shard_map(
        per_device,
        mesh=mesh,
        in_specs=placed,
        out_specs=(P("blk"), P("blk"), P("blk", "rep"), P("blk", "rep")),
        check_vma=False,
    )
```

```python
import functools
import math

import jax
import jax.numpy as jnp
from jax import lax
from jax.experimental import pallas as pl
from jax.experimental.pallas import tpu as pltpu
from jax.sharding import PartitionSpec as P

D = 512
BLOCK = 512
LANES = 128
GROUPS = BLOCK // LANES
TILES = 9
PAIR_DEV = 4
OFFSETS = (-1, 1, -2, 2)
MIRROR = (1, 0, 3, 2)
PEERS = 9

epsilon = 0.05
K2 = 1.0 / (epsilon * math.log(2.0))
INV_LN2 = 1.0 / math.log(2.0)
NEG = -1.0e30
MESH = pl.DeviceIdType.MESH


def kernel(
    n, pair_ref, owner_ref, x_hbm, y_hbm, m1_ref, m2_ref, f0_ref, g0_ref,
    f_out, g_out, mx_out, my_out,
    own, win, scores, bvec, bias, mpart, spart, lrow, lcol, acol, acc, obuf,
    pot, nrm, lmass, first, ibuf, home_part, part, part_in, tile, tile_in,
    load_sem, bsend, brecv, csend, crecv, isend, irecv, ipair,
    qsend, qrecv, qpair_send, qpair_recv, psend, precv, ppair, osend, orecv,
):
    i = lax.axis_index("blk")
    r = lax.axis_index("rep")
    other = 1 - r
    near = 1 - r

    def chip(offset):
        return lax.rem(i + (n + offset), n)

    ahead = chip(2 * r - 1)

    def rdma(src, dst, send, recv, where):
        return pltpu.make_async_remote_copy(
            src_ref=src, dst_ref=dst, send_sem=send, recv_sem=recv,
            device_id=where, device_id_type=MESH,
        )

    peers = [(chip(o), q) for o in OFFSETS for q in range(2)] + [(i, other)]
    barrier = pltpu.get_barrier_semaphore()
    for peer in peers:
        pl.semaphore_signal(barrier, inc=1, device_id=peer, device_id_type=MESH)
    load_y = pltpu.make_async_copy(y_hbm, own.at[0], load_sem.at[0])
    load_x = pltpu.make_async_copy(x_hbm, own.at[1], load_sem.at[1])
    load_y.start()
    load_x.start()
    pl.semaphore_wait(barrier, PEERS)

    def near_copy(t, c):
        return rdma(
            own.at[t, c], win.at[t, near, c], bsend.at[t, 0, c], brecv.at[t, 0, c], (ahead, r)
        )

    def far_copy(t, c):
        return rdma(
            win.at[t, near, c], win.at[t, 2 + near, c],
            bsend.at[t, 1, c], brecv.at[t, 1, c], (ahead, r),
        )

    def cross_copy(t, far, c, slot):
        at = win.at[t, 2 * far + slot, c]
        return rdma(at, at, csend.at[t, far, c], crecv.at[t, far, c], (i, other))

    def message(src, dst, send, recv, kk, q):
        where = (chip((1 - 2 * r) * (1 + kk)), q)
        return rdma(src, dst.at[r + 2 * kk], send.at[kk, q], recv.at[r + 2 * kk], where)

    load_y.wait()
    near_copy(0, 0).start()
    near_copy(0, 1).start()
    load_x.wait()

    pot[0] = g0_ref[r]
    pot[1] = f0_ref[r]
    lmass[0] = jnp.log(m2_ref[r]) * INV_LN2
    lmass[1] = jnp.log(m1_ref[r]) * INV_LN2

    def spread(row, store):
        for l in range(GROUPS):
            store[l : l + 1, :] = row[:, l * LANES : (l + 1) * LANES]

    for t in range(2):
        def square(g, _):
            at = pl.ds(pl.multiple_of(g * 64, 64), 64)
            v = own[t, r, at, :].astype(jnp.float32)
            v = v * v
            total = v[:, 0:LANES]
            for l in range(1, GROUPS):
                total = total + v[:, l * LANES : (l + 1) * LANES]
            mpart[at, :] = total
            return 0

        lax.fori_loop(0, BLOCK // 64, square, 0)
        total = jnp.sum(jnp.transpose(mpart[...]), axis=0, keepdims=True)
        spread(total * (1.0 / D), lrow)
        nrm[t] = lrow[0:GROUPS, :]

    def vector(t):
        return K2 * (pot[t] - nrm[t]) + lmass[t]

    first[r, 0, 0:GROUPS, :] = vector(0)
    first[r, 0, GROUPS : 2 * GROUPS, :] = pot[0]

    line = lax.broadcasted_iota(jnp.int32, (8, LANES), 0)
    listed = jnp.zeros((8, LANES), jnp.float32)
    for p in range(PAIR_DEV):
        a_id = pair_ref[0, p]
        c_id = pair_ref[1, p]
        x_at = owner_ref[jnp.maximum(a_id, 0)]
        y_at = owner_ref[jnp.maximum(c_id, 0)]
        offset = lax.rem((y_at >> 1) - i + (n + 2), n) - 2
        slot = jnp.where(offset == -1, 0, jnp.where(offset == 1, 1, jnp.where(offset == -2, 2, 3)))
        at = jnp.where(a_id >= 0, slot * 2 + (y_at & 1), -1)
        amount = ((x_at & 1) + 1).astype(jnp.float32)
        listed = listed + jnp.where(line == at, amount, 0.0)
    first[r, 1] = listed

    def first_pair(core):
        return rdma(first.at[core], first.at[core], ipair.at[0], ipair.at[1], (i, other))

    def first_copy(kk, q):
        return message(first, ibuf, isend, irecv, kk, q)

    first_pair(r).start()

    def put_scores(side, p, keys):
        dot = lax.dot_general(
            own[1 - side, r], keys, (((1,), (1,)), ((), ())), preferred_element_type=jnp.float32
        )
        scores[side, p] = dot * (2.0 * K2 / D)

    def home_side(side, _):
        put_scores(side, 0, own[side, r])
        return 0

    lax.fori_loop(0, 2, home_side, 0)

    first_pair(other).wait_recv()
    for kk in range(2):
        for q in range(2):
            first_copy(kk, q).start()

    def allow(v, block):
        low = jnp.where(v == 1.0, 0.0, jnp.where(v == 3.0, 0.0, NEG))
        high = jnp.where(v >= 2.0, 0.0, NEG)
        if isinstance(block, int):
            return low if block == 0 else high
        return jnp.where(block == 0, low, high)

    bias[0] = allow(first[0, 1] + first[1, 1], r)

    def window_scores(side, slot):
        def one(c, _):
            put_scores(side, 1 + slot * 2 + c, win[side, slot, c])
            return 0

        lax.fori_loop(0, 2, one, 0)

    def turn_vector():
        v = vector(1)
        row = jnp.concatenate([v[l : l + 1, :] for l in range(GROUPS)], axis=1)
        acol[...] = jnp.transpose(jnp.broadcast_to(row, (LANES, BLOCK)))

    def column_part(p, store, extra):
        for l in range(GROUPS):
            lanes = slice(l * LANES, (l + 1) * LANES)

            def term(k):
                at = slice(k * 64, (k + 1) * 64)
                return scores[0, p, at, lanes] + acol[at, :]

            high = functools.reduce(jnp.maximum, [term(k) for k in range(8)])
            total = sum(jnp.exp2(term(k) - high) for k in range(8))
            top = jnp.max(high, axis=0, keepdims=True)
            total = jnp.sum(total * jnp.exp2(high - top), axis=0, keepdims=True)
            store[l : l + 1, :] = top if extra is None else top + extra
            store[GROUPS + l : GROUPS + l + 1, :] = total

    def window_parts(step, low, high):
        def one(j, _):
            column_part(j + 1, part.at[step, j // 2, j % 2, r], bias[0, pl.ds(j, 1), :])
            return 0

        lax.fori_loop(low, high, one, 0)

    def part_give(step, kk):
        for c in range(2):
            at = part.at[step, r + 2 * kk, c, r]
            rdma(
                at, at, qpair_send.at[step, kk, c], qpair_recv.at[step, kk, c], (i, other)
            ).start()

    def part_copy(step, kk, c):
        slot = 1 - r + 2 * kk
        return rdma(
            part.at[step, slot, c], part_in.at[step, r + 2 * kk],
            qsend.at[step, kk, c], qrecv.at[step, r + 2 * kk], (chip((1 - 2 * r) * (1 + kk)), c),
        )

    def part_got(step, kk, c):
        at = part.at[step, 1 - r + 2 * kk, c, other]
        return rdma(
            at, at, qpair_send.at[step, kk, c], qpair_recv.at[step, kk, c], (i, other)
        )

    def part_send(step, kk):
        for c in range(2):
            part_got(step, kk, c).wait_recv()
            part_copy(step, kk, c).start()

    def put_vector(side, home, source):
        for p in range(TILES):
            ref = home if p == 0 else source((p - 1) // 2, (p - 1) % 2)
            for l in range(GROUPS):
                row = ref[l : l + 1, :]
                if p > 0:
                    row = row + bias[side, p - 1 : p, :]
                at = (p * GROUPS + l) * LANES
                bvec[side, :, at : at + LANES] = jnp.broadcast_to(row, (8, LANES))

    def lse_pass(side, tiles=range(TILES), merge=False):
        def group(g, _):
            at = pl.ds(pl.multiple_of(g * 32, 32), 32)

            def term(o):
                b = bvec[side, :, o * LANES : (o + 1) * LANES]
                p, l = divmod(o, GROUPS)
                v = scores[side, p, at, l * LANES : (l + 1) * LANES]
                return v + jnp.concatenate([b] * 4, axis=0)

            spots = [p * GROUPS + l for p in tiles for l in range(GROUPS)]
            high = jnp.maximum(
                functools.reduce(jnp.maximum, [term(o) for o in spots[0::2]]),
                functools.reduce(jnp.maximum, [term(o) for o in spots[1::2]]),
            )
            if merge:
                high = jnp.maximum(high, mpart[at, :])
            total = sum(jnp.exp2(term(o) - high) for o in spots[0::2])
            total = total + sum(jnp.exp2(term(o) - high) for o in spots[1::2])
            if merge:
                total = total + spart[at, :] * jnp.exp2(mpart[at, :] - high)
            mpart[at, :] = high
            spart[at, :] = total
            return 0

        lax.fori_loop(0, BLOCK // 32, group, 0)

    def row_update():
        turned = jnp.transpose(mpart[...])
        high = jnp.max(turned, axis=0, keepdims=True)
        total = jnp.sum(jnp.transpose(spart[...]) * jnp.exp2(turned - high), axis=0, keepdims=True)
        spread(high + jnp.log(total) * INV_LN2, lrow)
        move(1, lrow[0:GROUPS, :])

    def move(t, lse):
        pot[t] = 0.5 * (pot[t] - lse * (1.0 / K2) + nrm[t])

    def column_update(step):
        for s in range(4):
            part_copy_wait(step, s)
        tops = [home_part[step, 0:GROUPS, :]]
        totals = [home_part[step, GROUPS : 2 * GROUPS, :]]
        for s in range(4):
            for a in range(2):
                tops.append(part_in[step, s, a, 0:GROUPS, :])
                totals.append(part_in[step, s, a, GROUPS : 2 * GROUPS, :])
        top = functools.reduce(jnp.maximum, tops)
        total = sum(v * jnp.exp2(h - top) for h, v in zip(tops, totals))
        move(0, top + jnp.log(total) * INV_LN2)

    def part_copy_wait(step, s):
        rdma(
            part_in.at[step, s], part_in.at[step, s], qsend.at[step, 0, 0],
            qrecv.at[step, s], (i, other),
        ).wait_recv()

    def tile_pair(m, core):
        at = tile.at[m, core]
        return rdma(at, at, ppair.at[m, 0], ppair.at[m, 1], (i, other))

    def tile_copy(m, kk, q):
        return message(tile.at[m], tile_in.at[m], psend.at[m], precv.at[m], kk, q)

    def send_tile(m, t):
        tile[m, r, 0:GROUPS, :] = vector(t)
        tile[m, r, GROUPS : 2 * GROUPS, :] = pot[t]
        tile_pair(m, r).start()

    def relay_tile(m):
        tile_pair(m, other).wait_recv()
        for kk in range(2):
            for q in range(2):
                tile_copy(m, kk, q).start()

    def take_tile(m, side):
        for s in range(4):
            at = tile_in.at[m, s]
            rdma(at, at, psend.at[m, 0, 0], precv.at[m, s], (i, other)).wait_recv()
        put_vector(side, tile.at[m, r], lambda s, q: tile_in.at[m, s, q])

    def first_take():
        for s in range(4):
            at = ibuf.at[s]
            rdma(at, at, isend.at[0, 0], irecv.at[s], (i, other)).wait_recv()
        for s in range(4):
            theirs = ibuf[s, 0, 1] + ibuf[s, 1, 1]
            at = MIRROR[s] * 2
            v = jnp.where(r == 0, theirs[at : at + 1, :], theirs[at + 1 : at + 2, :])
            for q in range(2):
                bias[1, 2 * s + q : 2 * s + q + 1, :] = allow(v, q)
        put_vector(0, first.at[r, 0], lambda s, q: ibuf.at[s, q, 0])

    def near_arrive(t, c):
        near_copy(t, c).wait_recv()
        far_copy(t, c).start()
        cross_copy(t, 0, c, near).start()

    def far_arrive(t, c):
        far_copy(t, c).wait_recv()
        cross_copy(t, 1, c, near).start()

    def crossed(t, far):
        for c in range(2):
            cross_copy(t, far, c, other_near).wait_recv()

    other_near = r

    turn_vector()
    column_part(0, home_part.at[0], None)
    near_arrive(0, 0)
    near_arrive(0, 1)
    near_copy(1, 0).start()
    near_copy(1, 1).start()
    window_scores(0, near)
    crossed(0, 0)
    window_scores(0, other_near)
    window_parts(0, 0, 4)
    part_give(0, 0)
    first_take()
    lse_pass(0, range(0, 5))
    part_send(0, 0)

    far_arrive(0, 0)
    far_arrive(0, 1)
    window_scores(0, 2 + near)
    crossed(0, 1)
    window_scores(0, 2 + other_near)
    window_parts(0, 4, 8)
    part_give(0, 1)
    lse_pass(0, range(5, 9), True)
    part_send(0, 1)
    row_update()
    turn_vector()
    column_part(0, home_part.at[1], None)
    window_parts(1, 0, 8)
    for kk in range(2):
        part_give(1, kk)
    near_arrive(1, 0)
    for kk in range(2):
        part_send(1, kk)

    column_update(0)
    send_tile(0, 0)
    relay_tile(0)
    near_arrive(1, 1)
    column_update(1)
    send_tile(1, 0)
    relay_tile(1)
    window_scores(1, near)
    crossed(1, 0)
    window_scores(1, other_near)

    take_tile(0, 0)
    lse_pass(0)
    row_update()
    send_tile(2, 1)
    f_out[r] = pot[1]
    g_out[r] = pot[0]
    g_out[other] = tile[1, other, GROUPS : 2 * GROUPS, :]
    relay_tile(2)
    f_out[other] = tile[2, other, GROUPS : 2 * GROUPS, :]
    take_tile(1, 0)

    def out_copy(side):
        dst = (mx_out, my_out)[side]
        return rdma(obuf.at[side], dst.at[r], osend.at[side], orecv.at[side], (i, other))

    def final(side, out_ref):
        lse_pass(side)

        def column(g, _):
            at = pl.ds(pl.multiple_of(g * 64, 64), 64)
            part = mpart[at, :]
            high = jnp.max(part, axis=1, keepdims=True)
            total = jnp.sum(spart[at, :] * jnp.exp2(part - high), axis=1, keepdims=True)
            lcol[at, :] = jnp.broadcast_to(high + jnp.log(total) * INV_LN2, (64, LANES))
            return 0

        lax.fori_loop(0, BLOCK // 64, column, 0)

        def weigh(p, keys):
            pieces = []
            for l in range(GROUPS):
                o = pl.multiple_of(p * BLOCK + l * LANES, LANES)
                v = scores[side, p, :, l * LANES : (l + 1) * LANES]
                v = v + bvec[side, 0:1, pl.ds(o, LANES)]
                pieces.append(jnp.exp2(v - lcol[...]).astype(jnp.bfloat16))
            return jnp.dot(
                jnp.concatenate(pieces, axis=1), keys, preferred_element_type=jnp.float32
            )

        acc[...] = weigh(0, own[side, r])

        def one(j, _):
            acc[...] += weigh(j + 1, win[side, j // 2, j % 2])
            return 0

        lax.fori_loop(0, 8, one, 0)
        half = D // 2
        low = acc[:, 0:half].astype(jnp.bfloat16)
        high = acc[:, half:D].astype(jnp.bfloat16)
        obuf[side] = jnp.where(r == 0, high, low)
        out_copy(side).start()
        out_ref[r] = jnp.where(r == 0, low, high)

    final(0, mx_out)
    far_arrive(1, 0)
    far_arrive(1, 1)
    window_scores(1, 2 + near)
    crossed(1, 1)
    window_scores(1, 2 + other_near)
    take_tile(2, 1)
    final(1, my_out)

    for side in range(2):
        dst = (mx_out, my_out)[side]
        rdma(
            obuf.at[side], dst.at[other], osend.at[side], orecv.at[side], (i, other)
        ).wait_recv()
        out_copy(side).wait_send()
    for t in range(2):
        for c in range(2):
            near_copy(t, c).wait_send()
            far_copy(t, c).wait_send()
            for far in range(2):
                cross_copy(t, far, c, near).wait_send()
    first_pair(r).wait_send()
    for m in range(3):
        tile_pair(m, r).wait_send()
    for kk in range(2):
        for q in range(2):
            first_copy(kk, q).wait_send()
            for m in range(3):
                tile_copy(m, kk, q).wait_send()
            for step in range(2):
                part_copy(step, kk, q).wait_send()
                at = part.at[step, r + 2 * kk, q, r]
                rdma(
                    at, at, qpair_send.at[step, kk, q], qpair_recv.at[step, kk, q], (i, other)
                ).wait_send()


def emit(*refs):
    sources, sinks, rooms, (come, go) = refs[0:4], refs[4:8], refs[8:12], refs[12:14]
    into = [pltpu.make_async_copy(sources[k], rooms[k], come.at[k]) for k in range(4)]
    out = [pltpu.make_async_copy(rooms[k], sinks[k], go.at[k]) for k in range(4)]
    for copy in into:
        copy.start()
    for k in range(4):
        into[k].wait()
        out[k].start()
    for copy in out:
        copy.wait()


def per_device(
    x_points, y_points, first_masses, second_masses, f_start, g_start, block_owner, pair_list
):
    n = lax.axis_size("blk")
    shape = (2, GROUPS, LANES)
    f32, bf16 = jnp.float32, jnp.bfloat16
    dma = pltpu.SemaphoreType.DMA
    smem = pl.BlockSpec(memory_space=pltpu.SMEM)
    vmem = pl.BlockSpec(memory_space=pltpu.VMEM)
    hbm = pl.BlockSpec(memory_space=pl.ANY)
    f, g, mx, my = pl.pallas_call(
        functools.partial(kernel, n),
        out_shape=(
            jax.ShapeDtypeStruct(shape, f32),
            jax.ShapeDtypeStruct(shape, f32),
            jax.ShapeDtypeStruct((2, BLOCK, D // 2), bf16),
            jax.ShapeDtypeStruct((2, BLOCK, D // 2), bf16),
        ),
        in_specs=[smem, smem, hbm, hbm, vmem, vmem, vmem, vmem],
        out_specs=(vmem, vmem, vmem, vmem),
        scratch_shapes=[
            pltpu.VMEM((2, 2, BLOCK, D), bf16),
            pltpu.VMEM((2, 4, 2, BLOCK, D), bf16),
            pltpu.VMEM((2, TILES, BLOCK, BLOCK), f32),
            pltpu.VMEM((2, 8, TILES * BLOCK), f32),
            pltpu.VMEM((2, 8, LANES), f32),
            pltpu.VMEM((BLOCK, LANES), f32),
            pltpu.VMEM((BLOCK, LANES), f32),
            pltpu.VMEM((8, LANES), f32),
            pltpu.VMEM((BLOCK, LANES), f32),
            pltpu.VMEM((BLOCK, LANES), f32),
            pltpu.VMEM((BLOCK, D), f32),
            pltpu.VMEM((2, BLOCK, D // 2), bf16),
            pltpu.VMEM(shape, f32),
            pltpu.VMEM(shape, f32),
            pltpu.VMEM(shape, f32),
            pltpu.VMEM((2, 2, 8, LANES), f32),
            pltpu.VMEM((4, 2, 2, 8, LANES), f32),
            pltpu.VMEM((2, 8, LANES), f32),
            pltpu.VMEM((2, 4, 2, 2, 8, LANES), f32),
            pltpu.VMEM((2, 4, 2, 8, LANES), f32),
            pltpu.VMEM((3, 2, 8, LANES), f32),
            pltpu.VMEM((3, 4, 2, 8, LANES), f32),
            dma((2,)),
            dma((2, 2, 2)),
            dma((2, 2, 2)),
            dma((2, 2, 2)),
            dma((2, 2, 2)),
            dma((2, 2)),
            dma((4,)),
            dma((2,)),
            dma((2, 2, 2)),
            dma((2, 4)),
            dma((2, 2, 2)),
            dma((2, 2, 2)),
            dma((3, 2, 2)),
            dma((3, 4)),
            dma((3, 2)),
            dma((2,)),
            dma((2,)),
        ],
        compiler_params=pltpu.CompilerParams(
            collective_id=0, has_side_effects=True, vmem_limit_bytes=63 * 1024 * 1024
        ),
    )(
        pair_list.T, block_owner, x_points.reshape(2, BLOCK, D), y_points.reshape(2, BLOCK, D),
        first_masses.reshape(shape), second_masses.reshape(shape),
        f_start.reshape(shape), g_start.reshape(shape),
    )
    f, g, mx, my = pl.pallas_call(
        emit,
        out_shape=tuple(jax.ShapeDtypeStruct(a.shape, a.dtype) for a in (f, g, mx, my)),
        in_specs=[hbm] * 4,
        out_specs=(hbm,) * 4,
        scratch_shapes=[pltpu.VMEM(a.shape, a.dtype) for a in (f, g, mx, my)] + [dma((4,))] * 2,
        compiler_params=pltpu.CompilerParams(vmem_limit_bytes=63 * 1024 * 1024),
    )(f, g, mx, my)
    rows = 2 * BLOCK
    return f.reshape(rows), g.reshape(rows), mx.reshape(rows, D // 2), my.reshape(rows, D // 2)


def solution(mesh):
    placed = (
        P("blk", None),
        P("blk", None),
        P("blk"),
        P("blk"),
        P("blk"),
        P("blk"),
        P(),
        P(("blk", "rep"), None),
    )
    return jax.shard_map(
        per_device,
        mesh=mesh,
        in_specs=placed,
        out_specs=(P("blk"), P("blk"), P("blk", "rep"), P("blk", "rep")),
        check_vma=False,
    )
```

```python
import functools
import math

import jax
import jax.numpy as jnp
from jax import lax
from jax.experimental import pallas as pl
from jax.experimental.pallas import tpu as pltpu
from jax.sharding import PartitionSpec as P

D = 512
BLOCK = 512
LANES = 128
GROUPS = BLOCK // LANES
TILES = 9
PAIR_DEV = 4
OFFSETS = (-1, 1, -2, 2)
MIRROR = (1, 0, 3, 2)
PEERS = 9

epsilon = 0.05
K2 = 1.0 / (epsilon * math.log(2.0))
INV_LN2 = 1.0 / math.log(2.0)
NEG = -1.0e30
MESH = pl.DeviceIdType.MESH


def kernel(
    n, pair_ref, owner_ref, x_hbm, y_hbm, m1_hbm, m2_hbm, f0_hbm, g0_hbm,
    f_out, g_out, mx_out, my_out,
    own, win, scores, bvec, bias, mpart, spart, lrow, lcol, acol, acc, obuf,
    kept, ended, begin, pot, nrm, lmass, first, ibuf, home_part, part, part_in, tile, tile_in,
    load_sem, bsend, brecv, csend, crecv, isend, irecv, ipair,
    qsend, qrecv, qpair_send, qpair_recv, psend, precv, ppair, osend, orecv, kept_sem,
):
    i = lax.axis_index("blk")
    r = lax.axis_index("rep")
    other = 1 - r
    near = 1 - r

    def chip(offset):
        return lax.rem(i + (n + offset), n)

    ahead = chip(2 * r - 1)

    def rdma(src, dst, send, recv, where):
        return pltpu.make_async_remote_copy(
            src_ref=src, dst_ref=dst, send_sem=send, recv_sem=recv,
            device_id=where, device_id_type=MESH,
        )

    peers = [(chip(o), q) for o in OFFSETS for q in range(2)] + [(i, other)]
    barrier = pltpu.get_barrier_semaphore()
    for peer in peers:
        pl.semaphore_signal(barrier, inc=1, device_id=peer, device_id_type=MESH)
    loads = [
        pltpu.make_async_copy((y_hbm, x_hbm)[t].at[c], own.at[t, c], load_sem.at[2 * t + c])
        for t in range(2)
        for c in range(2)
    ]
    for k, source in enumerate((g0_hbm, f0_hbm, m2_hbm, m1_hbm)):
        loads.append(pltpu.make_async_copy(source, begin.at[k], load_sem.at[4 + k]))
    for load in loads:
        load.start()
    pl.semaphore_wait(barrier, PEERS)

    def near_copy(t, c):
        return rdma(
            own.at[t, c], win.at[t, near, c], bsend.at[t, 0, c], brecv.at[t, 0, c], (ahead, r)
        )

    def far_copy(t, c):
        return rdma(
            win.at[t, near, c], win.at[t, 2 + near, c],
            bsend.at[t, 1, c], brecv.at[t, 1, c], (ahead, r),
        )

    def cross_copy(t, far, c, slot):
        at = win.at[t, 2 * far + slot, c]
        return rdma(at, at, csend.at[t, far, c], crecv.at[t, far, c], (i, other))

    def message(src, dst, send, recv, kk, q):
        where = (chip((1 - 2 * r) * (1 + kk)), q)
        return rdma(src, dst.at[r + 2 * kk], send.at[kk, q], recv.at[r + 2 * kk], where)

    for c in range(2):
        loads[c].wait()
        near_copy(0, c).start()
    for load in loads[2:]:
        load.wait()

    for t in range(2):
        pot[t] = begin[t, r]
        lmass[t] = jnp.log(begin[2 + t, r]) * INV_LN2

    def spread(row, store):
        for l in range(GROUPS):
            store[l : l + 1, :] = row[:, l * LANES : (l + 1) * LANES]

    for t in range(2):
        def square(g, _):
            at = pl.ds(pl.multiple_of(g * 64, 64), 64)
            v = own[t, r, at, :].astype(jnp.float32)
            v = v * v
            total = v[:, 0:LANES]
            for l in range(1, GROUPS):
                total = total + v[:, l * LANES : (l + 1) * LANES]
            mpart[at, :] = total
            return 0

        lax.fori_loop(0, BLOCK // 64, square, 0)
        total = jnp.sum(jnp.transpose(mpart[...]), axis=0, keepdims=True)
        spread(total * (1.0 / D), lrow)
        nrm[t] = lrow[0:GROUPS, :]

    def vector(t):
        return K2 * (pot[t] - nrm[t]) + lmass[t]

    first[r, 0, 0:GROUPS, :] = vector(0)
    first[r, 0, GROUPS : 2 * GROUPS, :] = pot[0]

    line = lax.broadcasted_iota(jnp.int32, (8, LANES), 0)
    listed = jnp.zeros((8, LANES), jnp.float32)
    for p in range(PAIR_DEV):
        a_id = pair_ref[0, p]
        c_id = pair_ref[1, p]
        x_at = owner_ref[jnp.maximum(a_id, 0)]
        y_at = owner_ref[jnp.maximum(c_id, 0)]
        offset = lax.rem((y_at >> 1) - i + (n + 2), n) - 2
        slot = jnp.where(offset == -1, 0, jnp.where(offset == 1, 1, jnp.where(offset == -2, 2, 3)))
        at = jnp.where(a_id >= 0, slot * 2 + (y_at & 1), -1)
        amount = ((x_at & 1) + 1).astype(jnp.float32)
        listed = listed + jnp.where(line == at, amount, 0.0)
    first[r, 1] = listed

    def first_pair(core):
        return rdma(first.at[core], first.at[core], ipair.at[0], ipair.at[1], (i, other))

    def first_copy(kk, q):
        return message(first, ibuf, isend, irecv, kk, q)

    first_pair(r).start()

    def put_scores(side, p, keys):
        dot = lax.dot_general(
            own[1 - side, r], keys, (((1,), (1,)), ((), ())), preferred_element_type=jnp.float32
        )
        scores[side, p] = dot * (2.0 * K2 / D)

    def home_side(side, _):
        put_scores(side, 0, own[side, r])
        return 0

    lax.fori_loop(0, 2, home_side, 0)

    first_pair(other).wait_recv()
    for kk in range(2):
        for q in range(2):
            first_copy(kk, q).start()

    def allow(v, block):
        low = jnp.where(v == 1.0, 0.0, jnp.where(v == 3.0, 0.0, NEG))
        high = jnp.where(v >= 2.0, 0.0, NEG)
        if isinstance(block, int):
            return low if block == 0 else high
        return jnp.where(block == 0, low, high)

    bias[0] = allow(first[0, 1] + first[1, 1], r)

    def window_scores(side, slot):
        def one(c, _):
            put_scores(side, 1 + slot * 2 + c, win[side, slot, c])
            return 0

        lax.fori_loop(0, 2, one, 0)

    def one_score(side, slot, c):
        def one(_, carry):
            put_scores(side, 1 + slot * 2 + c, win[side, slot, c])
            return carry

        one(0, 0)

    def turn_vector():
        v = vector(1)
        row = jnp.concatenate([v[l : l + 1, :] for l in range(GROUPS)], axis=1)
        acol[...] = jnp.transpose(jnp.broadcast_to(row, (LANES, BLOCK)))

    def column_part(p, store, extra):
        for l in range(GROUPS):
            lanes = slice(l * LANES, (l + 1) * LANES)

            def term(k):
                at = slice(k * 64, (k + 1) * 64)
                return scores[0, p, at, lanes] + acol[at, :]

            high = functools.reduce(jnp.maximum, [term(k) for k in range(8)])
            total = sum(jnp.exp2(term(k) - high) for k in range(8))
            top = jnp.max(high, axis=0, keepdims=True)
            total = jnp.sum(total * jnp.exp2(high - top), axis=0, keepdims=True)
            store[l : l + 1, :] = top if extra is None else top + extra
            store[GROUPS + l : GROUPS + l + 1, :] = total

    def window_parts(step, low, high, stride=1):
        def one(k, _):
            j = low + k * stride
            column_part(j + 1, part.at[step, j // 2, j % 2, r], bias[0, pl.ds(j, 1), :])
            return 0

        lax.fori_loop(0, (high - low + stride - 1) // stride, one, 0)

    def part_give(step, kk, blocks=(0, 1)):
        for c in blocks:
            at = part.at[step, r + 2 * kk, c, r]
            rdma(
                at, at, qpair_send.at[step, kk, c], qpair_recv.at[step, kk, c], (i, other)
            ).start()

    def part_copy(step, kk, c):
        slot = 1 - r + 2 * kk
        return rdma(
            part.at[step, slot, c], part_in.at[step, r + 2 * kk],
            qsend.at[step, kk, c], qrecv.at[step, r + 2 * kk], (chip((1 - 2 * r) * (1 + kk)), c),
        )

    def part_got(step, kk, c):
        at = part.at[step, 1 - r + 2 * kk, c, other]
        return rdma(
            at, at, qpair_send.at[step, kk, c], qpair_recv.at[step, kk, c], (i, other)
        )

    def part_send(step, kk):
        for c in range(2):
            part_got(step, kk, c).wait_recv()
            part_copy(step, kk, c).start()

    def put_vector(side, home, source):
        for p in range(TILES):
            ref = home if p == 0 else source((p - 1) // 2, (p - 1) % 2)
            for l in range(GROUPS):
                row = ref[l : l + 1, :]
                if p > 0:
                    row = row + bias[side, p - 1 : p, :]
                at = (p * GROUPS + l) * LANES
                bvec[side, :, at : at + LANES] = jnp.broadcast_to(row, (8, LANES))

    def lse_pass(side, tiles=range(TILES), merge=False):
        def group(g, _):
            at = pl.ds(pl.multiple_of(g * 64, 64), 64)

            def term(o):
                b = bvec[side, :, o * LANES : (o + 1) * LANES]
                p, l = divmod(o, GROUPS)
                v = scores[side, p, at, l * LANES : (l + 1) * LANES]
                return v + jnp.concatenate([b] * 8, axis=0)

            spots = [p * GROUPS + l for p in tiles for l in range(GROUPS)]
            high = jnp.maximum(
                functools.reduce(jnp.maximum, [term(o) for o in spots[0::2]]),
                functools.reduce(jnp.maximum, [term(o) for o in spots[1::2]]),
            )
            if merge:
                high = jnp.maximum(high, mpart[at, :])
            total = sum(jnp.exp2(term(o) - high) for o in spots[0::2])
            total = total + sum(jnp.exp2(term(o) - high) for o in spots[1::2])
            if merge:
                total = total + spart[at, :] * jnp.exp2(mpart[at, :] - high)
            mpart[at, :] = high
            spart[at, :] = total
            return 0

        lax.fori_loop(0, BLOCK // 64, group, 0)

    def row_update():
        turned = jnp.transpose(mpart[...])
        high = jnp.max(turned, axis=0, keepdims=True)
        total = jnp.sum(jnp.transpose(spart[...]) * jnp.exp2(turned - high), axis=0, keepdims=True)
        spread(high + jnp.log(total) * INV_LN2, lrow)
        move(1, lrow[0:GROUPS, :])

    def move(t, lse):
        pot[t] = 0.5 * (pot[t] - lse * (1.0 / K2) + nrm[t])

    def column_update(step):
        for s in range(4):
            part_copy_wait(step, s)
        tops = [home_part[step, 0:GROUPS, :]]
        totals = [home_part[step, GROUPS : 2 * GROUPS, :]]
        for s in range(4):
            for a in range(2):
                tops.append(part_in[step, s, a, 0:GROUPS, :])
                totals.append(part_in[step, s, a, GROUPS : 2 * GROUPS, :])
        top = functools.reduce(jnp.maximum, tops)
        total = sum(v * jnp.exp2(h - top) for h, v in zip(tops, totals))
        move(0, top + jnp.log(total) * INV_LN2)

    def part_copy_wait(step, s):
        rdma(
            part_in.at[step, s], part_in.at[step, s], qsend.at[step, 0, 0],
            qrecv.at[step, s], (i, other),
        ).wait_recv()

    def tile_pair(m, core):
        at = tile.at[m, core]
        return rdma(at, at, ppair.at[m, 0], ppair.at[m, 1], (i, other))

    def tile_copy(m, kk, q):
        return message(tile.at[m], tile_in.at[m], psend.at[m], precv.at[m], kk, q)

    def send_tile(m, t):
        tile[m, r, 0:GROUPS, :] = vector(t)
        tile[m, r, GROUPS : 2 * GROUPS, :] = pot[t]
        tile_pair(m, r).start()

    def relay_tile(m):
        tile_pair(m, other).wait_recv()
        for kk in range(2):
            for q in range(2):
                tile_copy(m, kk, q).start()

    def take_tile(m, side):
        for s in range(4):
            at = tile_in.at[m, s]
            rdma(at, at, psend.at[m, 0, 0], precv.at[m, s], (i, other)).wait_recv()
        put_vector(side, tile.at[m, r], lambda s, q: tile_in.at[m, s, q])

    def first_take():
        for s in range(4):
            at = ibuf.at[s]
            rdma(at, at, isend.at[0, 0], irecv.at[s], (i, other)).wait_recv()
        for s in range(4):
            theirs = ibuf[s, 0, 1] + ibuf[s, 1, 1]
            at = MIRROR[s] * 2
            v = jnp.where(r == 0, theirs[at : at + 1, :], theirs[at + 1 : at + 2, :])
            for q in range(2):
                bias[1, 2 * s + q : 2 * s + q + 1, :] = allow(v, q)
        put_vector(0, first.at[r, 0], lambda s, q: ibuf.at[s, q, 0])

    def near_arrive(t, c):
        near_copy(t, c).wait_recv()
        far_copy(t, c).start()
        cross_copy(t, 0, c, near).start()

    def far_arrive(t, c):
        far_copy(t, c).wait_recv()
        cross_copy(t, 1, c, near).start()

    def crossed(t, far, blocks=(0, 1)):
        for c in blocks:
            cross_copy(t, far, c, other_near).wait_recv()

    other_near = r

    def ended_copy(t):
        return pltpu.make_async_copy(ended.at[t], (g_out, f_out)[t], kept_sem.at[2 + t])

    def kept_copy(side):
        return pltpu.make_async_copy(
            kept.at[side], (mx_out, my_out)[side].at[r], kept_sem.at[side]
        )

    turn_vector()
    column_part(0, home_part.at[0], None)
    near_arrive(0, 0)
    near_arrive(0, 1)
    near_copy(1, 0).start()
    near_copy(1, 1).start()
    window_scores(0, near)
    crossed(0, 0)
    window_scores(0, other_near)
    window_parts(0, 0, 4)
    part_give(0, 0)
    first_take()
    lse_pass(0, range(0, 5))
    part_send(0, 0)

    far_arrive(0, 0)
    one_score(0, 2 + near, 0)
    crossed(0, 1, (0,))
    one_score(0, 2 + other_near, 0)
    window_parts(0, 4, 8, 2)
    part_give(0, 1, (0,))
    far_arrive(0, 1)
    one_score(0, 2 + near, 1)
    crossed(0, 1, (1,))
    one_score(0, 2 + other_near, 1)
    window_parts(0, 5, 8, 2)
    part_give(0, 1, (1,))
    part_send(0, 1)
    lse_pass(0, range(5, 9), True)
    row_update()
    turn_vector()
    column_part(0, home_part.at[1], None)
    window_parts(1, 0, 8)
    for kk in range(2):
        part_give(1, kk)
    near_arrive(1, 0)
    for kk in range(2):
        part_send(1, kk)

    column_update(0)
    send_tile(0, 0)
    relay_tile(0)
    near_arrive(1, 1)
    column_update(1)
    send_tile(1, 0)
    relay_tile(1)
    window_scores(1, near)
    crossed(1, 0)
    window_scores(1, other_near)

    take_tile(0, 0)
    lse_pass(0)
    row_update()
    send_tile(2, 1)
    relay_tile(2)
    for t in range(2):
        ended[t, r] = pot[t]
        ended[t, other] = tile[1 + t, other, GROUPS : 2 * GROUPS, :]
        ended_copy(t).start()
    take_tile(1, 0)

    def out_copy(side):
        dst = (mx_out, my_out)[side]
        return rdma(obuf.at[side], dst.at[r], osend.at[side], orecv.at[side], (i, other))

    def final(side):
        lse_pass(side)

        def column(g, _):
            at = pl.ds(pl.multiple_of(g * 64, 64), 64)
            part = mpart[at, :]
            high = jnp.max(part, axis=1, keepdims=True)
            total = jnp.sum(spart[at, :] * jnp.exp2(part - high), axis=1, keepdims=True)
            lcol[at, :] = jnp.broadcast_to(high + jnp.log(total) * INV_LN2, (64, LANES))
            return 0

        lax.fori_loop(0, BLOCK // 64, column, 0)

        def weigh(first_tile, count, keys):
            pieces = []
            for k in range(count):
                p = first_tile + k
                for l in range(GROUPS):
                    o = pl.multiple_of(p * BLOCK + l * LANES, LANES)
                    v = scores[side, p, :, l * LANES : (l + 1) * LANES]
                    v = v + bvec[side, 0:1, pl.ds(o, LANES)]
                    pieces.append(jnp.exp2(v - lcol[...]).astype(jnp.bfloat16))
            return jnp.dot(
                jnp.concatenate(pieces, axis=1), keys, preferred_element_type=jnp.float32
            )

        acc[...] = weigh(0, 1, own[side, r])

        acc[...] += weigh(1, 8, win[side].reshape(8 * BLOCK, D))
        half = D // 2
        low = acc[:, 0:half].astype(jnp.bfloat16)
        high = acc[:, half:D].astype(jnp.bfloat16)
        obuf[side] = jnp.where(r == 0, high, low)
        out_copy(side).start()
        kept[side] = jnp.where(r == 0, low, high)
        kept_copy(side).start()

    final(0)
    for c in range(2):
        far_arrive(1, c)
    window_scores(1, 2 + near)
    crossed(1, 1)
    window_scores(1, 2 + other_near)
    take_tile(2, 1)
    final(1)

    for side in range(2):
        dst = (mx_out, my_out)[side]
        rdma(
            obuf.at[side], dst.at[other], osend.at[side], orecv.at[side], (i, other)
        ).wait_recv()
        out_copy(side).wait_send()
        kept_copy(side).wait()
        ended_copy(side).wait()
    for t in range(2):
        for c in range(2):
            near_copy(t, c).wait_send()
            far_copy(t, c).wait_send()
            for far in range(2):
                cross_copy(t, far, c, near).wait_send()
    first_pair(r).wait_send()
    for m in range(3):
        tile_pair(m, r).wait_send()
    for kk in range(2):
        for q in range(2):
            first_copy(kk, q).wait_send()
            for m in range(3):
                tile_copy(m, kk, q).wait_send()
            for step in range(2):
                part_copy(step, kk, q).wait_send()
                at = part.at[step, r + 2 * kk, q, r]
                rdma(
                    at, at, qpair_send.at[step, kk, q], qpair_recv.at[step, kk, q], (i, other)
                ).wait_send()


def emit(*refs):
    sources, sinks, rooms, (come, go) = refs[0:4], refs[4:8], refs[8:12], refs[12:14]
    into = [pltpu.make_async_copy(sources[k], rooms[k], come.at[k]) for k in range(4)]
    out = [pltpu.make_async_copy(rooms[k], sinks[k], go.at[k]) for k in range(4)]
    for copy in into:
        copy.start()
    for k in range(4):
        into[k].wait()
        out[k].start()
    for copy in out:
        copy.wait()


def per_device(
    x_points, y_points, first_masses, second_masses, f_start, g_start, block_owner, pair_list
):
    n = lax.axis_size("blk")
    shape = (2, GROUPS, LANES)
    f32, bf16 = jnp.float32, jnp.bfloat16
    dma = pltpu.SemaphoreType.DMA
    smem = pl.BlockSpec(memory_space=pltpu.SMEM)
    hbm = pl.BlockSpec(memory_space=pl.ANY)
    f, g, mx, my = pl.pallas_call(
        functools.partial(kernel, n),
        out_shape=(
            jax.ShapeDtypeStruct(shape, f32),
            jax.ShapeDtypeStruct(shape, f32),
            jax.ShapeDtypeStruct((2, BLOCK, D // 2), bf16),
            jax.ShapeDtypeStruct((2, BLOCK, D // 2), bf16),
        ),
        in_specs=[smem, smem] + [hbm] * 6,
        out_specs=(hbm,) * 4,
        scratch_shapes=[
            pltpu.VMEM((2, 2, BLOCK, D), bf16),
            pltpu.VMEM((2, 4, 2, BLOCK, D), bf16),
            pltpu.VMEM((2, TILES, BLOCK, BLOCK), f32),
            pltpu.VMEM((2, 8, TILES * BLOCK), f32),
            pltpu.VMEM((2, 8, LANES), f32),
            pltpu.VMEM((BLOCK, LANES), f32),
            pltpu.VMEM((BLOCK, LANES), f32),
            pltpu.VMEM((8, LANES), f32),
            pltpu.VMEM((BLOCK, LANES), f32),
            pltpu.VMEM((BLOCK, LANES), f32),
            pltpu.VMEM((BLOCK, D), f32),
            pltpu.VMEM((2, BLOCK, D // 2), bf16),
            pltpu.VMEM((2, BLOCK, D // 2), bf16),
            pltpu.VMEM((2,) + shape, f32),
            pltpu.VMEM((4,) + shape, f32),
            pltpu.VMEM(shape, f32),
            pltpu.VMEM(shape, f32),
            pltpu.VMEM(shape, f32),
            pltpu.VMEM((2, 2, 8, LANES), f32),
            pltpu.VMEM((4, 2, 2, 8, LANES), f32),
            pltpu.VMEM((2, 8, LANES), f32),
            pltpu.VMEM((2, 4, 2, 2, 8, LANES), f32),
            pltpu.VMEM((2, 4, 2, 8, LANES), f32),
            pltpu.VMEM((3, 2, 8, LANES), f32),
            pltpu.VMEM((3, 4, 2, 8, LANES), f32),
            dma((8,)),
            dma((2, 2, 2)),
            dma((2, 2, 2)),
            dma((2, 2, 2)),
            dma((2, 2, 2)),
            dma((2, 2)),
            dma((4,)),
            dma((2,)),
            dma((2, 2, 2)),
            dma((2, 4)),
            dma((2, 2, 2)),
            dma((2, 2, 2)),
            dma((3, 2, 2)),
            dma((3, 4)),
            dma((3, 2)),
            dma((2,)),
            dma((2,)),
            dma((4,)),
        ],
        compiler_params=pltpu.CompilerParams(
            collective_id=0, has_side_effects=True, vmem_limit_bytes=63 * 1024 * 1024
        ),
    )(
        pair_list.T, block_owner, x_points.reshape(2, BLOCK, D), y_points.reshape(2, BLOCK, D),
        first_masses.reshape(shape), second_masses.reshape(shape),
        f_start.reshape(shape), g_start.reshape(shape),
    )
    f, g, mx, my = pl.pallas_call(
        emit,
        out_shape=tuple(jax.ShapeDtypeStruct(a.shape, a.dtype) for a in (f, g, mx, my)),
        in_specs=[hbm] * 4,
        out_specs=(hbm,) * 4,
        scratch_shapes=[pltpu.VMEM(a.shape, a.dtype) for a in (f, g, mx, my)] + [dma((4,))] * 2,
        compiler_params=pltpu.CompilerParams(vmem_limit_bytes=63 * 1024 * 1024),
    )(f, g, mx, my)
    rows = 2 * BLOCK
    return f.reshape(rows), g.reshape(rows), mx.reshape(rows, D // 2), my.reshape(rows, D // 2)


def solution(mesh):
    placed = (
        P("blk", None),
        P("blk", None),
        P("blk"),
        P("blk"),
        P("blk"),
        P("blk"),
        P(),
        P(("blk", "rep"), None),
    )
    return jax.shard_map(
        per_device,
        mesh=mesh,
        in_specs=placed,
        out_specs=(P("blk"), P("blk"), P("blk", "rep"), P("blk", "rep")),
        check_vma=False,
    )
```

```python
import functools
import math

import jax
import jax.numpy as jnp
from jax import lax
from jax.experimental import pallas as pl
from jax.experimental.pallas import tpu as pltpu
from jax.sharding import PartitionSpec as P

D = 512
BLOCK = 512
LANES = 128
GROUPS = BLOCK // LANES
TILES = 9
PAIR_DEV = 4
OFFSETS = (-1, 1, -2, 2)
MIRROR = (1, 0, 3, 2)
PEERS = 9

epsilon = 0.05
K2 = 1.0 / (epsilon * math.log(2.0))
INV_LN2 = 1.0 / math.log(2.0)
NEG = -1.0e30
MESH = pl.DeviceIdType.MESH


def kernel(
    n, pair_ref, owner_ref, x_hbm, y_hbm, m1_hbm, m2_hbm, f0_hbm, g0_hbm,
    f_out, g_out, mx_out, my_out,
    own, win, scores, bvec, bias, mpart, spart, lrow, lcol, acol, obuf,
    kept, ended, begin, pot, nrm, lmass, first, ibuf, home_part, part, part_in, tile, tile_in,
    load_sem, bsend, brecv, csend, crecv, isend, irecv, ipair,
    qsend, qrecv, qpair_send, qpair_recv, psend, precv, ppair, osend, orecv, kept_sem,
):
    i = lax.axis_index("blk")
    r = lax.axis_index("rep")
    other = 1 - r
    near = 1 - r

    def chip(offset):
        return lax.rem(i + (n + offset), n)

    ahead = chip(2 * r - 1)

    def rdma(src, dst, send, recv, where):
        return pltpu.make_async_remote_copy(
            src_ref=src, dst_ref=dst, send_sem=send, recv_sem=recv,
            device_id=where, device_id_type=MESH,
        )

    peers = [(chip(o), q) for o in OFFSETS for q in range(2)] + [(i, other)]
    barrier = pltpu.get_barrier_semaphore()
    for peer in peers:
        pl.semaphore_signal(barrier, inc=1, device_id=peer, device_id_type=MESH)
    loads = [
        pltpu.make_async_copy((y_hbm, x_hbm)[t].at[c], own.at[t, c], load_sem.at[2 * t + c])
        for t in range(2)
        for c in range(2)
    ]
    for k, source in enumerate((g0_hbm, f0_hbm, m2_hbm, m1_hbm)):
        loads.append(pltpu.make_async_copy(source, begin.at[k], load_sem.at[4 + k]))
    for load in loads:
        load.start()
    pl.semaphore_wait(barrier, PEERS)

    def near_copy(t, c):
        return rdma(
            own.at[t, c], win.at[t, near, c], bsend.at[t, 0, c], brecv.at[t, 0, c], (ahead, r)
        )

    def far_copy(t, c):
        return rdma(
            win.at[t, near, c], win.at[t, 2 + near, c],
            bsend.at[t, 1, c], brecv.at[t, 1, c], (ahead, r),
        )

    def cross_copy(t, far, c, slot):
        at = win.at[t, 2 * far + slot, c]
        return rdma(at, at, csend.at[t, far, c], crecv.at[t, far, c], (i, other))

    def message(src, dst, send, recv, kk, q):
        where = (chip((1 - 2 * r) * (1 + kk)), q)
        return rdma(src, dst.at[r + 2 * kk], send.at[kk, q], recv.at[r + 2 * kk], where)

    for c in range(2):
        loads[c].wait()
        near_copy(0, c).start()
    for load in loads[2:]:
        load.wait()

    for t in range(2):
        pot[t] = begin[t, r]
        lmass[t] = jnp.log(begin[2 + t, r]) * INV_LN2

    def spread(row, store):
        for l in range(GROUPS):
            store[l : l + 1, :] = row[:, l * LANES : (l + 1) * LANES]

    for t in range(2):
        def square(g, _):
            at = pl.ds(pl.multiple_of(g * 64, 64), 64)
            v = own[t, r, at, :].astype(jnp.float32)
            v = v * v
            total = v[:, 0:LANES]
            for l in range(1, GROUPS):
                total = total + v[:, l * LANES : (l + 1) * LANES]
            mpart[at, :] = total
            return 0

        lax.fori_loop(0, BLOCK // 64, square, 0)
        total = jnp.sum(jnp.transpose(mpart[...]), axis=0, keepdims=True)
        spread(total * (1.0 / D), lrow)
        nrm[t] = lrow[0:GROUPS, :]

    def vector(t):
        return K2 * (pot[t] - nrm[t]) + lmass[t]

    first[r, 0, 0:GROUPS, :] = vector(0)
    first[r, 0, GROUPS : 2 * GROUPS, :] = pot[0]

    line = lax.broadcasted_iota(jnp.int32, (8, LANES), 0)
    listed = jnp.zeros((8, LANES), jnp.float32)
    for p in range(PAIR_DEV):
        a_id = pair_ref[0, p]
        c_id = pair_ref[1, p]
        x_at = owner_ref[jnp.maximum(a_id, 0)]
        y_at = owner_ref[jnp.maximum(c_id, 0)]
        offset = lax.rem((y_at >> 1) - i + (n + 2), n) - 2
        slot = jnp.where(offset == -1, 0, jnp.where(offset == 1, 1, jnp.where(offset == -2, 2, 3)))
        at = jnp.where(a_id >= 0, slot * 2 + (y_at & 1), -1)
        amount = ((x_at & 1) + 1).astype(jnp.float32)
        listed = listed + jnp.where(line == at, amount, 0.0)
    first[r, 1] = listed

    def first_pair(core):
        return rdma(first.at[core], first.at[core], ipair.at[0], ipair.at[1], (i, other))

    def first_copy(kk, q):
        return message(first, ibuf, isend, irecv, kk, q)

    first_pair(r).start()

    def put_scores(side, p, keys):
        dot = lax.dot_general(
            own[1 - side, r], keys, (((1,), (1,)), ((), ())), preferred_element_type=jnp.float32
        )
        scores[side, p] = dot * (2.0 * K2 / D)

    def home_side(side, _):
        put_scores(side, 0, own[side, r])
        return 0

    lax.fori_loop(0, 2, home_side, 0)

    first_pair(other).wait_recv()
    for kk in range(2):
        for q in range(2):
            first_copy(kk, q).start()

    def allow(v, block):
        low = jnp.where(v == 1.0, 0.0, jnp.where(v == 3.0, 0.0, NEG))
        high = jnp.where(v >= 2.0, 0.0, NEG)
        if isinstance(block, int):
            return low if block == 0 else high
        return jnp.where(block == 0, low, high)

    bias[0] = allow(first[0, 1] + first[1, 1], r)

    def window_scores(side, slot):
        def one(c, _):
            put_scores(side, 1 + slot * 2 + c, win[side, slot, c])
            return 0

        lax.fori_loop(0, 2, one, 0)

    def one_score(side, slot, c):
        def one(_, carry):
            put_scores(side, 1 + slot * 2 + c, win[side, slot, c])
            return carry

        one(0, 0)

    def turn_vector():
        v = vector(1)
        row = jnp.concatenate([v[l : l + 1, :] for l in range(GROUPS)], axis=1)
        acol[...] = jnp.transpose(jnp.broadcast_to(row, (LANES, BLOCK)))

    def column_part(p, store, extra):
        for l in range(GROUPS):
            lanes = slice(l * LANES, (l + 1) * LANES)

            def term(k):
                at = slice(k * 64, (k + 1) * 64)
                return scores[0, p, at, lanes] + acol[at, :]

            high = functools.reduce(jnp.maximum, [term(k) for k in range(8)])
            total = sum(jnp.exp2(term(k) - high) for k in range(8))
            top = jnp.max(high, axis=0, keepdims=True)
            total = jnp.sum(total * jnp.exp2(high - top), axis=0, keepdims=True)
            store[l : l + 1, :] = top if extra is None else top + extra
            store[GROUPS + l : GROUPS + l + 1, :] = total

    def window_parts(step, low, high, stride=1):
        def one(k, _):
            j = low + k * stride
            column_part(j + 1, part.at[step, j // 2, j % 2, r], bias[0, pl.ds(j, 1), :])
            return 0

        lax.fori_loop(0, (high - low + stride - 1) // stride, one, 0)

    def part_give(step, kk, blocks=(0, 1)):
        for c in blocks:
            at = part.at[step, r + 2 * kk, c, r]
            rdma(
                at, at, qpair_send.at[step, kk, c], qpair_recv.at[step, kk, c], (i, other)
            ).start()

    def part_copy(step, kk, c):
        slot = 1 - r + 2 * kk
        return rdma(
            part.at[step, slot, c], part_in.at[step, r + 2 * kk],
            qsend.at[step, kk, c], qrecv.at[step, r + 2 * kk], (chip((1 - 2 * r) * (1 + kk)), c),
        )

    def part_got(step, kk, c):
        at = part.at[step, 1 - r + 2 * kk, c, other]
        return rdma(
            at, at, qpair_send.at[step, kk, c], qpair_recv.at[step, kk, c], (i, other)
        )

    def part_send(step, kk):
        for c in range(2):
            part_got(step, kk, c).wait_recv()
            part_copy(step, kk, c).start()

    def put_vector(side, home, source):
        for p in range(TILES):
            ref = home if p == 0 else source((p - 1) // 2, (p - 1) % 2)
            for l in range(GROUPS):
                row = ref[l : l + 1, :]
                if p > 0:
                    row = row + bias[side, p - 1 : p, :]
                at = (p * GROUPS + l) * LANES
                bvec[side, :, at : at + LANES] = jnp.broadcast_to(row, (8, LANES))

    def lse_pass(side, tiles=range(TILES), merge=False):
        def group(g, _):
            at = pl.ds(pl.multiple_of(g * 64, 64), 64)

            def term(o):
                b = bvec[side, :, o * LANES : (o + 1) * LANES]
                p, l = divmod(o, GROUPS)
                v = scores[side, p, at, l * LANES : (l + 1) * LANES]
                return v + jnp.concatenate([b] * 8, axis=0)

            spots = [p * GROUPS + l for p in tiles for l in range(GROUPS)]
            high = jnp.maximum(
                functools.reduce(jnp.maximum, [term(o) for o in spots[0::2]]),
                functools.reduce(jnp.maximum, [term(o) for o in spots[1::2]]),
            )
            if merge:
                high = jnp.maximum(high, mpart[at, :])
            total = sum(jnp.exp2(term(o) - high) for o in spots[0::2])
            total = total + sum(jnp.exp2(term(o) - high) for o in spots[1::2])
            if merge:
                total = total + spart[at, :] * jnp.exp2(mpart[at, :] - high)
            mpart[at, :] = high
            spart[at, :] = total
            return 0

        lax.fori_loop(0, BLOCK // 64, group, 0)

    def row_update():
        turned = jnp.transpose(mpart[...])
        high = jnp.max(turned, axis=0, keepdims=True)
        total = jnp.sum(jnp.transpose(spart[...]) * jnp.exp2(turned - high), axis=0, keepdims=True)
        spread(high + jnp.log(total) * INV_LN2, lrow)
        move(1, lrow[0:GROUPS, :])

    def move(t, lse):
        pot[t] = 0.5 * (pot[t] - lse * (1.0 / K2) + nrm[t])

    def column_update(step):
        for s in range(4):
            part_copy_wait(step, s)
        tops = [home_part[step, 0:GROUPS, :]]
        totals = [home_part[step, GROUPS : 2 * GROUPS, :]]
        for s in range(4):
            for a in range(2):
                tops.append(part_in[step, s, a, 0:GROUPS, :])
                totals.append(part_in[step, s, a, GROUPS : 2 * GROUPS, :])
        top = functools.reduce(jnp.maximum, tops)
        total = sum(v * jnp.exp2(h - top) for h, v in zip(tops, totals))
        move(0, top + jnp.log(total) * INV_LN2)

    def part_copy_wait(step, s):
        rdma(
            part_in.at[step, s], part_in.at[step, s], qsend.at[step, 0, 0],
            qrecv.at[step, s], (i, other),
        ).wait_recv()

    def tile_pair(m, core):
        at = tile.at[m, core]
        return rdma(at, at, ppair.at[m, 0], ppair.at[m, 1], (i, other))

    def tile_copy(m, kk, q):
        return message(tile.at[m], tile_in.at[m], psend.at[m], precv.at[m], kk, q)

    def send_tile(m, t):
        tile[m, r, 0:GROUPS, :] = vector(t)
        tile[m, r, GROUPS : 2 * GROUPS, :] = pot[t]
        tile_pair(m, r).start()

    def relay_tile(m):
        tile_pair(m, other).wait_recv()
        for kk in range(2):
            for q in range(2):
                tile_copy(m, kk, q).start()

    def take_tile(m, side):
        for s in range(4):
            at = tile_in.at[m, s]
            rdma(at, at, psend.at[m, 0, 0], precv.at[m, s], (i, other)).wait_recv()
        put_vector(side, tile.at[m, r], lambda s, q: tile_in.at[m, s, q])

    def first_take():
        for s in range(4):
            at = ibuf.at[s]
            rdma(at, at, isend.at[0, 0], irecv.at[s], (i, other)).wait_recv()
        for s in range(4):
            theirs = ibuf[s, 0, 1] + ibuf[s, 1, 1]
            at = MIRROR[s] * 2
            v = jnp.where(r == 0, theirs[at : at + 1, :], theirs[at + 1 : at + 2, :])
            for q in range(2):
                bias[1, 2 * s + q : 2 * s + q + 1, :] = allow(v, q)
        put_vector(0, first.at[r, 0], lambda s, q: ibuf.at[s, q, 0])

    def near_arrive(t, c):
        near_copy(t, c).wait_recv()
        far_copy(t, c).start()
        cross_copy(t, 0, c, near).start()

    def far_arrive(t, c):
        far_copy(t, c).wait_recv()
        cross_copy(t, 1, c, near).start()

    def crossed(t, far, blocks=(0, 1)):
        for c in blocks:
            cross_copy(t, far, c, other_near).wait_recv()

    other_near = r

    def ended_copy(t):
        return pltpu.make_async_copy(ended.at[t], (g_out, f_out)[t], kept_sem.at[2 + t])

    def kept_copy(side):
        return pltpu.make_async_copy(
            kept.at[side], (mx_out, my_out)[side].at[r], kept_sem.at[side]
        )

    turn_vector()
    column_part(0, home_part.at[0], None)
    near_arrive(0, 0)
    near_arrive(0, 1)
    near_copy(1, 0).start()
    near_copy(1, 1).start()
    window_scores(0, near)
    crossed(0, 0)
    window_scores(0, other_near)
    window_parts(0, 0, 4)
    part_give(0, 0)
    first_take()
    lse_pass(0, range(0, 5))
    part_send(0, 0)

    far_arrive(0, 0)
    one_score(0, 2 + near, 0)
    crossed(0, 1, (0,))
    one_score(0, 2 + other_near, 0)
    window_parts(0, 4, 8, 2)
    part_give(0, 1, (0,))
    far_arrive(0, 1)
    one_score(0, 2 + near, 1)
    crossed(0, 1, (1,))
    one_score(0, 2 + other_near, 1)
    window_parts(0, 5, 8, 2)
    part_give(0, 1, (1,))
    part_send(0, 1)
    lse_pass(0, range(5, 9), True)
    row_update()
    turn_vector()
    window_parts(1, 4, 8)
    part_give(1, 1)
    window_parts(1, 0, 4)
    part_give(1, 0)
    part_send(1, 1)
    near_arrive(1, 0)
    part_send(1, 0)
    column_part(0, home_part.at[1], None)

    column_update(0)
    send_tile(0, 0)
    relay_tile(0)
    near_arrive(1, 1)
    column_update(1)
    send_tile(1, 0)
    relay_tile(1)
    window_scores(1, near)
    crossed(1, 0)
    window_scores(1, other_near)

    take_tile(0, 0)
    lse_pass(0)
    row_update()
    send_tile(2, 1)
    take_tile(1, 0)
    relay_tile(2)
    for t in range(2):
        ended[t, r] = pot[t]
        ended[t, other] = tile[1 + t, other, GROUPS : 2 * GROUPS, :]
        ended_copy(t).start()

    def out_copy(side):
        dst = (mx_out, my_out)[side]
        return rdma(obuf.at[side], dst.at[r], osend.at[side], orecv.at[side], (i, other))

    def final(side):
        lse_pass(side)

        def column(g, _):
            at = pl.ds(pl.multiple_of(g * 64, 64), 64)
            part = mpart[at, :]
            high = jnp.max(part, axis=1, keepdims=True)
            total = jnp.sum(spart[at, :] * jnp.exp2(part - high), axis=1, keepdims=True)
            lcol[at, :] = jnp.broadcast_to(high + jnp.log(total) * INV_LN2, (64, LANES))
            return 0

        lax.fori_loop(0, BLOCK // 64, column, 0)

        def weigh(first_tile, count, keys):
            pieces = []
            for k in range(count):
                p = first_tile + k
                for l in range(GROUPS):
                    o = pl.multiple_of(p * BLOCK + l * LANES, LANES)
                    v = scores[side, p, :, l * LANES : (l + 1) * LANES]
                    v = v + bvec[side, 0:1, pl.ds(o, LANES)]
                    pieces.append(jnp.exp2(v - lcol[...]).astype(jnp.bfloat16))
            return jnp.dot(
                jnp.concatenate(pieces, axis=1), keys, preferred_element_type=jnp.float32
            )

        total = weigh(0, 1, own[side, r]) + weigh(1, 8, win[side].reshape(8 * BLOCK, D))
        half = D // 2
        low = total[:, 0:half].astype(jnp.bfloat16)
        high = total[:, half:D].astype(jnp.bfloat16)
        obuf[side] = jnp.where(r == 0, high, low)
        out_copy(side).start()
        kept[side] = jnp.where(r == 0, low, high)
        kept_copy(side).start()

    final(0)
    for c in range(2):
        far_arrive(1, c)
    window_scores(1, 2 + near)
    crossed(1, 1)
    window_scores(1, 2 + other_near)
    take_tile(2, 1)
    final(1)

    for side in range(2):
        dst = (mx_out, my_out)[side]
        rdma(
            obuf.at[side], dst.at[other], osend.at[side], orecv.at[side], (i, other)
        ).wait_recv()
        out_copy(side).wait_send()
        kept_copy(side).wait()
        ended_copy(side).wait()
    for t in range(2):
        for c in range(2):
            near_copy(t, c).wait_send()
            far_copy(t, c).wait_send()
            for far in range(2):
                cross_copy(t, far, c, near).wait_send()
    first_pair(r).wait_send()
    for m in range(3):
        tile_pair(m, r).wait_send()
    for kk in range(2):
        for q in range(2):
            first_copy(kk, q).wait_send()
            for m in range(3):
                tile_copy(m, kk, q).wait_send()
            for step in range(2):
                part_copy(step, kk, q).wait_send()
                at = part.at[step, r + 2 * kk, q, r]
                rdma(
                    at, at, qpair_send.at[step, kk, q], qpair_recv.at[step, kk, q], (i, other)
                ).wait_send()


def emit(*refs):
    sources, sinks, rooms, (come, go) = refs[0:4], refs[4:8], refs[8:12], refs[12:14]
    into = [pltpu.make_async_copy(sources[k], rooms[k], come.at[k]) for k in range(4)]
    out = [pltpu.make_async_copy(rooms[k], sinks[k], go.at[k]) for k in range(4)]
    for copy in into:
        copy.start()
    for k in range(4):
        into[k].wait()
        out[k].start()
    for copy in out:
        copy.wait()


def per_device(
    x_points, y_points, first_masses, second_masses, f_start, g_start, block_owner, pair_list
):
    n = lax.axis_size("blk")
    shape = (2, GROUPS, LANES)
    f32, bf16 = jnp.float32, jnp.bfloat16
    dma = pltpu.SemaphoreType.DMA
    smem = pl.BlockSpec(memory_space=pltpu.SMEM)
    hbm = pl.BlockSpec(memory_space=pl.ANY)
    f, g, mx, my = pl.pallas_call(
        functools.partial(kernel, n),
        out_shape=(
            jax.ShapeDtypeStruct(shape, f32),
            jax.ShapeDtypeStruct(shape, f32),
            jax.ShapeDtypeStruct((2, BLOCK, D // 2), bf16),
            jax.ShapeDtypeStruct((2, BLOCK, D // 2), bf16),
        ),
        in_specs=[smem, smem] + [hbm] * 6,
        out_specs=(hbm,) * 4,
        scratch_shapes=[
            pltpu.VMEM((2, 2, BLOCK, D), bf16),
            pltpu.VMEM((2, 4, 2, BLOCK, D), bf16),
            pltpu.VMEM((2, TILES, BLOCK, BLOCK), f32),
            pltpu.VMEM((2, 8, TILES * BLOCK), f32),
            pltpu.VMEM((2, 8, LANES), f32),
            pltpu.VMEM((BLOCK, LANES), f32),
            pltpu.VMEM((BLOCK, LANES), f32),
            pltpu.VMEM((8, LANES), f32),
            pltpu.VMEM((BLOCK, LANES), f32),
            pltpu.VMEM((BLOCK, LANES), f32),
            pltpu.VMEM((2, BLOCK, D // 2), bf16),
            pltpu.VMEM((2, BLOCK, D // 2), bf16),
            pltpu.VMEM((2,) + shape, f32),
            pltpu.VMEM((4,) + shape, f32),
            pltpu.VMEM(shape, f32),
            pltpu.VMEM(shape, f32),
            pltpu.VMEM(shape, f32),
            pltpu.VMEM((2, 2, 8, LANES), f32),
            pltpu.VMEM((4, 2, 2, 8, LANES), f32),
            pltpu.VMEM((2, 8, LANES), f32),
            pltpu.VMEM((2, 4, 2, 2, 8, LANES), f32),
            pltpu.VMEM((2, 4, 2, 8, LANES), f32),
            pltpu.VMEM((3, 2, 8, LANES), f32),
            pltpu.VMEM((3, 4, 2, 8, LANES), f32),
            dma((8,)),
            dma((2, 2, 2)),
            dma((2, 2, 2)),
            dma((2, 2, 2)),
            dma((2, 2, 2)),
            dma((2, 2)),
            dma((4,)),
            dma((2,)),
            dma((2, 2, 2)),
            dma((2, 4)),
            dma((2, 2, 2)),
            dma((2, 2, 2)),
            dma((3, 2, 2)),
            dma((3, 4)),
            dma((3, 2)),
            dma((2,)),
            dma((2,)),
            dma((4,)),
        ],
        compiler_params=pltpu.CompilerParams(
            collective_id=0, has_side_effects=True, vmem_limit_bytes=63 * 1024 * 1024
        ),
    )(
        pair_list.T, block_owner, x_points.reshape(2, BLOCK, D), y_points.reshape(2, BLOCK, D),
        first_masses.reshape(shape), second_masses.reshape(shape),
        f_start.reshape(shape), g_start.reshape(shape),
    )
    f, g, mx, my = pl.pallas_call(
        emit,
        out_shape=tuple(jax.ShapeDtypeStruct(a.shape, a.dtype) for a in (f, g, mx, my)),
        in_specs=[hbm] * 4,
        out_specs=(hbm,) * 4,
        scratch_shapes=[pltpu.VMEM(a.shape, a.dtype) for a in (f, g, mx, my)] + [dma((4,))] * 2,
        compiler_params=pltpu.CompilerParams(vmem_limit_bytes=63 * 1024 * 1024),
    )(f, g, mx, my)
    rows = 2 * BLOCK
    return f.reshape(rows), g.reshape(rows), mx.reshape(rows, D // 2), my.reshape(rows, D // 2)


def solution(mesh):
    placed = (
        P("blk", None),
        P("blk", None),
        P("blk"),
        P("blk"),
        P("blk"),
        P("blk"),
        P(),
        P(("blk", "rep"), None),
    )
    return jax.shard_map(
        per_device,
        mesh=mesh,
        in_specs=placed,
        out_specs=(P("blk"), P("blk"), P("blk", "rep"), P("blk", "rep")),
        check_vma=False,
    )
```

```python
import functools
import math

import jax
import jax.numpy as jnp
from jax import lax
from jax.experimental import pallas as pl
from jax.experimental.pallas import tpu as pltpu
from jax.sharding import PartitionSpec as P

D = 512
BLOCK = 512
LANES = 128
GROUPS = BLOCK // LANES
TILES = 9
PAIR_DEV = 4
OFFSETS = (-1, 1, -2, 2)
MIRROR = (1, 0, 3, 2)
PEERS = 9

epsilon = 0.05
K2 = 1.0 / (epsilon * math.log(2.0))
INV_LN2 = 1.0 / math.log(2.0)
NEG = -1.0e30
MESH = pl.DeviceIdType.MESH


def kernel(
    n, pair_ref, owner_ref, x_hbm, y_hbm, m1_hbm, m2_hbm, f0_hbm, g0_hbm,
    f_out, g_out, mx_out, my_out,
    own, win, scores, bvec, bias, mpart, spart, lrow, lcol, acol, obuf,
    kept, ended, begin, pot, nrm, lmass, first, ibuf, home_part, part, part_in, tile, tile_in,
    load_sem, bsend, brecv, csend, crecv, isend, irecv, ipair,
    qsend, qrecv, qpair_send, qpair_recv, psend, precv, ppair, osend, orecv, kept_sem,
):
    i = lax.axis_index("blk")
    r = lax.axis_index("rep")
    other = 1 - r
    near = 1 - r

    def chip(offset):
        return lax.rem(i + (n + offset), n)

    ahead = chip(2 * r - 1)

    def rdma(src, dst, send, recv, where):
        return pltpu.make_async_remote_copy(
            src_ref=src, dst_ref=dst, send_sem=send, recv_sem=recv,
            device_id=where, device_id_type=MESH,
        )

    peers = [(chip(o), q) for o in OFFSETS for q in range(2)] + [(i, other)]
    barrier = pltpu.get_barrier_semaphore()
    for peer in peers:
        pl.semaphore_signal(barrier, inc=1, device_id=peer, device_id_type=MESH)
    loads = [
        pltpu.make_async_copy((y_hbm, x_hbm)[t].at[c], own.at[t, c], load_sem.at[2 * t + c])
        for t in range(2)
        for c in range(2)
    ]
    for k, source in enumerate((g0_hbm, f0_hbm, m2_hbm, m1_hbm)):
        loads.append(pltpu.make_async_copy(source, begin.at[k], load_sem.at[4 + k]))
    for load in loads:
        load.start()
    pl.semaphore_wait(barrier, PEERS)

    def near_copy(t, c):
        return rdma(
            own.at[t, c], win.at[t, near, c], bsend.at[t, 0, c], brecv.at[t, 0, c], (ahead, r)
        )

    def far_copy(t, c):
        return rdma(
            win.at[t, near, c], win.at[t, 2 + near, c],
            bsend.at[t, 1, c], brecv.at[t, 1, c], (ahead, r),
        )

    def cross_copy(t, far, c, slot):
        at = win.at[t, 2 * far + slot, c]
        return rdma(at, at, csend.at[t, far, c], crecv.at[t, far, c], (i, other))

    def message(src, dst, send, recv, kk, q):
        where = (chip((1 - 2 * r) * (1 + kk)), q)
        return rdma(src, dst.at[r + 2 * kk], send.at[kk, q], recv.at[r + 2 * kk], where)

    for c in range(2):
        loads[c].wait()
        near_copy(0, c).start()
    for load in loads[2:]:
        load.wait()

    for t in range(2):
        pot[t] = begin[t, r]
        lmass[t] = jnp.log(begin[2 + t, r]) * INV_LN2

    def spread(row, store):
        for l in range(GROUPS):
            store[l : l + 1, :] = row[:, l * LANES : (l + 1) * LANES]

    for t in range(2):
        def square(g, _):
            at = pl.ds(pl.multiple_of(g * 64, 64), 64)
            v = own[t, r, at, :].astype(jnp.float32)
            v = v * v
            total = v[:, 0:LANES]
            for l in range(1, GROUPS):
                total = total + v[:, l * LANES : (l + 1) * LANES]
            mpart[at, :] = total
            return 0

        lax.fori_loop(0, BLOCK // 64, square, 0)
        total = jnp.sum(jnp.transpose(mpart[...]), axis=0, keepdims=True)
        spread(total * (1.0 / D), lrow)
        nrm[t] = lrow[0:GROUPS, :]

    def vector(t):
        return K2 * (pot[t] - nrm[t]) + lmass[t]

    first[r, 0, 0:GROUPS, :] = vector(0)
    first[r, 0, GROUPS : 2 * GROUPS, :] = pot[0]

    line = lax.broadcasted_iota(jnp.int32, (8, LANES), 0)
    listed = jnp.zeros((8, LANES), jnp.float32)
    for p in range(PAIR_DEV):
        a_id = pair_ref[0, p]
        c_id = pair_ref[1, p]
        x_at = owner_ref[jnp.maximum(a_id, 0)]
        y_at = owner_ref[jnp.maximum(c_id, 0)]
        offset = lax.rem((y_at >> 1) - i + (n + 2), n) - 2
        slot = jnp.where(offset == -1, 0, jnp.where(offset == 1, 1, jnp.where(offset == -2, 2, 3)))
        at = jnp.where(a_id >= 0, slot * 2 + (y_at & 1), -1)
        amount = ((x_at & 1) + 1).astype(jnp.float32)
        listed = listed + jnp.where(line == at, amount, 0.0)
    first[r, 1] = listed

    def first_pair(core):
        return rdma(first.at[core], first.at[core], ipair.at[0], ipair.at[1], (i, other))

    def first_copy(kk, q):
        return message(first, ibuf, isend, irecv, kk, q)

    first_pair(r).start()

    def put_scores(side, p, keys):
        dot = lax.dot_general(
            own[1 - side, r], keys, (((1,), (1,)), ((), ())), preferred_element_type=jnp.float32
        )
        scores[side, p] = dot * (2.0 * K2 / D)

    def home_side(side, _):
        put_scores(side, 0, own[side, r])
        return 0

    lax.fori_loop(0, 2, home_side, 0)

    first_pair(other).wait_recv()
    for kk in range(2):
        for q in range(2):
            first_copy(kk, q).start()

    def allow(v, block):
        low = jnp.where(v == 1.0, 0.0, jnp.where(v == 3.0, 0.0, NEG))
        high = jnp.where(v >= 2.0, 0.0, NEG)
        if isinstance(block, int):
            return low if block == 0 else high
        return jnp.where(block == 0, low, high)

    bias[0] = allow(first[0, 1] + first[1, 1], r)

    def window_scores(side, slot):
        def one(c, _):
            put_scores(side, 1 + slot * 2 + c, win[side, slot, c])
            return 0

        lax.fori_loop(0, 2, one, 0)

    def one_score(side, slot, c):
        def one(_, carry):
            put_scores(side, 1 + slot * 2 + c, win[side, slot, c])
            return carry

        one(0, 0)

    def turn_vector():
        v = vector(1)
        row = jnp.concatenate([v[l : l + 1, :] for l in range(GROUPS)], axis=1)
        acol[...] = jnp.transpose(jnp.broadcast_to(row, (LANES, BLOCK)))

    def column_part(p, store, extra):
        for l in range(GROUPS):
            lanes = slice(l * LANES, (l + 1) * LANES)

            def term(k):
                at = slice(k * 64, (k + 1) * 64)
                return scores[0, p, at, lanes] + acol[at, :]

            high = functools.reduce(jnp.maximum, [term(k) for k in range(8)])
            total = sum(jnp.exp2(term(k) - high) for k in range(8))
            top = jnp.max(high, axis=0, keepdims=True)
            total = jnp.sum(total * jnp.exp2(high - top), axis=0, keepdims=True)
            store[l : l + 1, :] = top if extra is None else top + extra
            store[GROUPS + l : GROUPS + l + 1, :] = total

    def window_parts(step, low, high, stride=1):
        def one(k, _):
            j = low + k * stride
            column_part(j + 1, part.at[step, j // 2, j % 2, r], bias[0, pl.ds(j, 1), :])
            return 0

        lax.fori_loop(0, (high - low + stride - 1) // stride, one, 0)

    def part_give(step, kk, blocks=(0, 1)):
        for c in blocks:
            at = part.at[step, r + 2 * kk, c, r]
            rdma(
                at, at, qpair_send.at[step, kk, c], qpair_recv.at[step, kk, c], (i, other)
            ).start()

    def part_copy(step, kk, c):
        slot = 1 - r + 2 * kk
        return rdma(
            part.at[step, slot, c], part_in.at[step, r + 2 * kk],
            qsend.at[step, kk, c], qrecv.at[step, r + 2 * kk], (chip((1 - 2 * r) * (1 + kk)), c),
        )

    def part_got(step, kk, c):
        at = part.at[step, 1 - r + 2 * kk, c, other]
        return rdma(
            at, at, qpair_send.at[step, kk, c], qpair_recv.at[step, kk, c], (i, other)
        )

    def part_send(step, kk):
        for c in range(2):
            part_got(step, kk, c).wait_recv()
            part_copy(step, kk, c).start()

    def put_vector(side, home, source):
        for p in range(TILES):
            ref = home if p == 0 else source((p - 1) // 2, (p - 1) % 2)
            for l in range(GROUPS):
                row = ref[l : l + 1, :]
                if p > 0:
                    row = row + bias[side, p - 1 : p, :]
                at = (p * GROUPS + l) * LANES
                bvec[side, :, at : at + LANES] = jnp.broadcast_to(row, (8, LANES))

    def lse_pass(side, tiles=range(TILES), merge=False):
        def group(g, _):
            at = pl.ds(pl.multiple_of(g * 128, 128), 128)

            def term(o):
                b = bvec[side, :, o * LANES : (o + 1) * LANES]
                p, l = divmod(o, GROUPS)
                v = scores[side, p, at, l * LANES : (l + 1) * LANES]
                return v + jnp.concatenate([b] * 16, axis=0)

            spots = [p * GROUPS + l for p in tiles for l in range(GROUPS)]
            high = jnp.maximum(
                functools.reduce(jnp.maximum, [term(o) for o in spots[0::2]]),
                functools.reduce(jnp.maximum, [term(o) for o in spots[1::2]]),
            )
            if merge:
                high = jnp.maximum(high, mpart[at, :])
            total = sum(jnp.exp2(term(o) - high) for o in spots[0::2])
            total = total + sum(jnp.exp2(term(o) - high) for o in spots[1::2])
            if merge:
                total = total + spart[at, :] * jnp.exp2(mpart[at, :] - high)
            mpart[at, :] = high
            spart[at, :] = total
            return 0

        lax.fori_loop(0, BLOCK // 128, group, 0)

    def row_update():
        turned = jnp.transpose(mpart[...])
        high = jnp.max(turned, axis=0, keepdims=True)
        total = jnp.sum(jnp.transpose(spart[...]) * jnp.exp2(turned - high), axis=0, keepdims=True)
        spread(high + jnp.log(total) * INV_LN2, lrow)
        move(1, lrow[0:GROUPS, :])

    def move(t, lse):
        pot[t] = 0.5 * (pot[t] - lse * (1.0 / K2) + nrm[t])

    def column_update(step):
        for s in range(4):
            part_copy_wait(step, s)
        tops = [home_part[step, 0:GROUPS, :]]
        totals = [home_part[step, GROUPS : 2 * GROUPS, :]]
        for s in range(4):
            for a in range(2):
                tops.append(part_in[step, s, a, 0:GROUPS, :])
                totals.append(part_in[step, s, a, GROUPS : 2 * GROUPS, :])
        top = functools.reduce(jnp.maximum, tops)
        total = sum(v * jnp.exp2(h - top) for h, v in zip(tops, totals))
        move(0, top + jnp.log(total) * INV_LN2)

    def part_copy_wait(step, s):
        rdma(
            part_in.at[step, s], part_in.at[step, s], qsend.at[step, 0, 0],
            qrecv.at[step, s], (i, other),
        ).wait_recv()

    def tile_pair(m, core):
        at = tile.at[m, core]
        return rdma(at, at, ppair.at[m, 0], ppair.at[m, 1], (i, other))

    def tile_copy(m, kk, q):
        return message(tile.at[m], tile_in.at[m], psend.at[m], precv.at[m], kk, q)

    def send_tile(m, t):
        tile[m, r, 0:GROUPS, :] = vector(t)
        tile[m, r, GROUPS : 2 * GROUPS, :] = pot[t]
        tile_pair(m, r).start()

    def relay_tile(m):
        tile_pair(m, other).wait_recv()
        for kk in range(2):
            for q in range(2):
                tile_copy(m, kk, q).start()

    def take_tile(m, side):
        for s in range(4):
            at = tile_in.at[m, s]
            rdma(at, at, psend.at[m, 0, 0], precv.at[m, s], (i, other)).wait_recv()
        put_vector(side, tile.at[m, r], lambda s, q: tile_in.at[m, s, q])

    def first_take():
        for s in range(4):
            at = ibuf.at[s]
            rdma(at, at, isend.at[0, 0], irecv.at[s], (i, other)).wait_recv()
        for s in range(4):
            theirs = ibuf[s, 0, 1] + ibuf[s, 1, 1]
            at = MIRROR[s] * 2
            v = jnp.where(r == 0, theirs[at : at + 1, :], theirs[at + 1 : at + 2, :])
            for q in range(2):
                bias[1, 2 * s + q : 2 * s + q + 1, :] = allow(v, q)
        put_vector(0, first.at[r, 0], lambda s, q: ibuf.at[s, q, 0])

    def near_arrive(t, c):
        near_copy(t, c).wait_recv()
        far_copy(t, c).start()
        cross_copy(t, 0, c, near).start()

    def far_arrive(t, c):
        far_copy(t, c).wait_recv()
        cross_copy(t, 1, c, near).start()

    def crossed(t, far, blocks=(0, 1)):
        for c in blocks:
            cross_copy(t, far, c, other_near).wait_recv()

    other_near = r

    def ended_copy(t):
        return pltpu.make_async_copy(ended.at[t], (g_out, f_out)[t], kept_sem.at[2 + t])

    def kept_copy(side):
        return pltpu.make_async_copy(
            kept.at[side], (mx_out, my_out)[side].at[r], kept_sem.at[side]
        )

    turn_vector()
    column_part(0, home_part.at[0], None)
    near_arrive(0, 0)
    near_arrive(0, 1)
    near_copy(1, 0).start()
    near_copy(1, 1).start()
    window_scores(0, near)
    crossed(0, 0)
    window_scores(0, other_near)
    window_parts(0, 0, 4)
    part_give(0, 0)
    first_take()
    lse_pass(0, range(0, 5))
    part_send(0, 0)

    far_arrive(0, 0)
    one_score(0, 2 + near, 0)
    crossed(0, 1, (0,))
    one_score(0, 2 + other_near, 0)
    window_parts(0, 4, 8, 2)
    part_give(0, 1, (0,))
    far_arrive(0, 1)
    one_score(0, 2 + near, 1)
    crossed(0, 1, (1,))
    one_score(0, 2 + other_near, 1)
    window_parts(0, 5, 8, 2)
    part_give(0, 1, (1,))
    part_send(0, 1)
    lse_pass(0, range(5, 9), True)
    row_update()
    turn_vector()
    window_parts(1, 4, 8)
    part_give(1, 1)
    window_parts(1, 0, 4)
    part_give(1, 0)
    part_send(1, 1)
    near_arrive(1, 0)
    part_send(1, 0)
    column_part(0, home_part.at[1], None)

    column_update(0)
    send_tile(0, 0)
    relay_tile(0)
    near_arrive(1, 1)
    column_update(1)
    send_tile(1, 0)
    relay_tile(1)
    window_scores(1, near)
    crossed(1, 0)
    window_scores(1, other_near)

    take_tile(0, 0)
    lse_pass(0)
    row_update()
    send_tile(2, 1)
    take_tile(1, 0)
    relay_tile(2)
    for t in range(2):
        ended[t, r] = pot[t]
        ended[t, other] = tile[1 + t, other, GROUPS : 2 * GROUPS, :]
        ended_copy(t).start()

    def out_copy(side):
        dst = (mx_out, my_out)[side]
        return rdma(obuf.at[side], dst.at[r], osend.at[side], orecv.at[side], (i, other))

    def final(side):
        lse_pass(side)

        def column(g, _):
            at = pl.ds(pl.multiple_of(g * 64, 64), 64)
            part = mpart[at, :]
            high = jnp.max(part, axis=1, keepdims=True)
            total = jnp.sum(spart[at, :] * jnp.exp2(part - high), axis=1, keepdims=True)
            lcol[at, :] = jnp.broadcast_to(high + jnp.log(total) * INV_LN2, (64, LANES))
            return 0

        lax.fori_loop(0, BLOCK // 64, column, 0)

        def weigh(first_tile, count, keys):
            pieces = []
            for k in range(count):
                p = first_tile + k
                for l in range(GROUPS):
                    o = pl.multiple_of(p * BLOCK + l * LANES, LANES)
                    v = scores[side, p, :, l * LANES : (l + 1) * LANES]
                    v = v + bvec[side, 0:1, pl.ds(o, LANES)]
                    pieces.append(jnp.exp2(v - lcol[...]).astype(jnp.bfloat16))
            return jnp.dot(
                jnp.concatenate(pieces, axis=1), keys, preferred_element_type=jnp.float32
            )

        total = weigh(0, 1, own[side, r]) + weigh(1, 8, win[side].reshape(8 * BLOCK, D))
        half = D // 2
        low = total[:, 0:half].astype(jnp.bfloat16)
        high = total[:, half:D].astype(jnp.bfloat16)
        obuf[side] = jnp.where(r == 0, high, low)
        out_copy(side).start()
        kept[side] = jnp.where(r == 0, low, high)
        kept_copy(side).start()

    final(0)
    for c in range(2):
        far_arrive(1, c)
    window_scores(1, 2 + near)
    crossed(1, 1)
    window_scores(1, 2 + other_near)
    take_tile(2, 1)
    final(1)

    for side in range(2):
        dst = (mx_out, my_out)[side]
        rdma(
            obuf.at[side], dst.at[other], osend.at[side], orecv.at[side], (i, other)
        ).wait_recv()
        out_copy(side).wait_send()
        kept_copy(side).wait()
        ended_copy(side).wait()
    for t in range(2):
        for c in range(2):
            near_copy(t, c).wait_send()
            far_copy(t, c).wait_send()
            for far in range(2):
                cross_copy(t, far, c, near).wait_send()
    first_pair(r).wait_send()
    for m in range(3):
        tile_pair(m, r).wait_send()
    for kk in range(2):
        for q in range(2):
            first_copy(kk, q).wait_send()
            for m in range(3):
                tile_copy(m, kk, q).wait_send()
            for step in range(2):
                part_copy(step, kk, q).wait_send()
                at = part.at[step, r + 2 * kk, q, r]
                rdma(
                    at, at, qpair_send.at[step, kk, q], qpair_recv.at[step, kk, q], (i, other)
                ).wait_send()


def emit(*refs):
    sources, sinks, rooms, (come, go) = refs[0:4], refs[4:8], refs[8:12], refs[12:14]
    into = [pltpu.make_async_copy(sources[k], rooms[k], come.at[k]) for k in range(4)]
    out = [pltpu.make_async_copy(rooms[k], sinks[k], go.at[k]) for k in range(4)]
    for copy in into:
        copy.start()
    for k in range(4):
        into[k].wait()
        out[k].start()
    for copy in out:
        copy.wait()


def per_device(
    x_points, y_points, first_masses, second_masses, f_start, g_start, block_owner, pair_list
):
    n = lax.axis_size("blk")
    shape = (2, GROUPS, LANES)
    f32, bf16 = jnp.float32, jnp.bfloat16
    dma = pltpu.SemaphoreType.DMA
    smem = pl.BlockSpec(memory_space=pltpu.SMEM)
    hbm = pl.BlockSpec(memory_space=pl.ANY)
    f, g, mx, my = pl.pallas_call(
        functools.partial(kernel, n),
        out_shape=(
            jax.ShapeDtypeStruct(shape, f32),
            jax.ShapeDtypeStruct(shape, f32),
            jax.ShapeDtypeStruct((2, BLOCK, D // 2), bf16),
            jax.ShapeDtypeStruct((2, BLOCK, D // 2), bf16),
        ),
        in_specs=[smem, smem] + [hbm] * 6,
        out_specs=(hbm,) * 4,
        scratch_shapes=[
            pltpu.VMEM((2, 2, BLOCK, D), bf16),
            pltpu.VMEM((2, 4, 2, BLOCK, D), bf16),
            pltpu.VMEM((2, TILES, BLOCK, BLOCK), f32),
            pltpu.VMEM((2, 8, TILES * BLOCK), f32),
            pltpu.VMEM((2, 8, LANES), f32),
            pltpu.VMEM((BLOCK, LANES), f32),
            pltpu.VMEM((BLOCK, LANES), f32),
            pltpu.VMEM((8, LANES), f32),
            pltpu.VMEM((BLOCK, LANES), f32),
            pltpu.VMEM((BLOCK, LANES), f32),
            pltpu.VMEM((2, BLOCK, D // 2), bf16),
            pltpu.VMEM((2, BLOCK, D // 2), bf16),
            pltpu.VMEM((2,) + shape, f32),
            pltpu.VMEM((4,) + shape, f32),
            pltpu.VMEM(shape, f32),
            pltpu.VMEM(shape, f32),
            pltpu.VMEM(shape, f32),
            pltpu.VMEM((2, 2, 8, LANES), f32),
            pltpu.VMEM((4, 2, 2, 8, LANES), f32),
            pltpu.VMEM((2, 8, LANES), f32),
            pltpu.VMEM((2, 4, 2, 2, 8, LANES), f32),
            pltpu.VMEM((2, 4, 2, 8, LANES), f32),
            pltpu.VMEM((3, 2, 8, LANES), f32),
            pltpu.VMEM((3, 4, 2, 8, LANES), f32),
            dma((8,)),
            dma((2, 2, 2)),
            dma((2, 2, 2)),
            dma((2, 2, 2)),
            dma((2, 2, 2)),
            dma((2, 2)),
            dma((4,)),
            dma((2,)),
            dma((2, 2, 2)),
            dma((2, 4)),
            dma((2, 2, 2)),
            dma((2, 2, 2)),
            dma((3, 2, 2)),
            dma((3, 4)),
            dma((3, 2)),
            dma((2,)),
            dma((2,)),
            dma((4,)),
        ],
        compiler_params=pltpu.CompilerParams(
            collective_id=0, has_side_effects=True, vmem_limit_bytes=63 * 1024 * 1024
        ),
    )(
        pair_list.T, block_owner, x_points.reshape(2, BLOCK, D), y_points.reshape(2, BLOCK, D),
        first_masses.reshape(shape), second_masses.reshape(shape),
        f_start.reshape(shape), g_start.reshape(shape),
    )
    f, g, mx, my = pl.pallas_call(
        emit,
        out_shape=tuple(jax.ShapeDtypeStruct(a.shape, a.dtype) for a in (f, g, mx, my)),
        in_specs=[hbm] * 4,
        out_specs=(hbm,) * 4,
        scratch_shapes=[pltpu.VMEM(a.shape, a.dtype) for a in (f, g, mx, my)] + [dma((4,))] * 2,
        compiler_params=pltpu.CompilerParams(vmem_limit_bytes=63 * 1024 * 1024),
    )(f, g, mx, my)
    rows = 2 * BLOCK
    return f.reshape(rows), g.reshape(rows), mx.reshape(rows, D // 2), my.reshape(rows, D // 2)


def solution(mesh):
    placed = (
        P("blk", None),
        P("blk", None),
        P("blk"),
        P("blk"),
        P("blk"),
        P("blk"),
        P(),
        P(("blk", "rep"), None),
    )
    return jax.shard_map(
        per_device,
        mesh=mesh,
        in_specs=placed,
        out_specs=(P("blk"), P("blk"), P("blk", "rep"), P("blk", "rep")),
        check_vma=False,
    )
```
